256 devices in a mesh: half: 2 (over core), row: 16 (over x, y), col: 8 (over z).
Axes of the slice: x: 4, y: 4, z: 8, core: 2. Of those that a mesh axis runs over, the one named last changes fastest.
Arguments:
- particles: bfloat16 [512, 2, 64, 4096], P(('half', 'row', 'col')), may hold values from -9 to 9
- orient_bin: int32 [512], P(('half', 'row', 'col')), may hold values from 0 to 15
- tilt_slope: int32 [512, 2], P(('half', 'row', 'col')), may hold values from 12 to 40
- interp_table: bfloat16 [16, 3, 64, 64], replicated, may hold values from 0 to 1.6, as said below
Outputs:
- half_maps: float32 [2, 2, 64, 4096], P('half', None, 'row', 'col')
- shell_power: float32 [2, 29], replicated
- shell_correlation: float32 [2, 29], P('half')
The draws below stay inside these ranges and needn't reach their ends.
Inputs may be any that keep to these rules, and one draw needn't show every extreme that they name: `interp_table`: nonnegative entries.
All inputs are finite; a program needn't handle non-finite values.
Results may differ from the reference program's by a relative error of at most 0.00063.
Values sent between devices are 32-bit elements; how exact they have to be, the bound alone decides.
A program may use at most 64 MiB of HBM per device.

```python
import jax
import jax.numpy as jnp
from jax import lax

GRID = 64
BINS = 16
SHELLS = 29
PARTICLES = 512


def draw_particles(key, part):
    full_shape = (PARTICLES, 2, GRID, GRID * GRID)
    signal = jax.random.normal(jax.random.fold_in(key, 11), (1, 2, GRID, GRID * GRID), jnp.float32)
    noise_part = jax.random.normal(key, full_shape, jnp.float32)
    combined = 0.7 * signal + noise_part
    return jnp.clip(combined, -9.0, 9.0).astype(jnp.bfloat16)


def draw_interp_table(key, part):
    full_shape = (BINS, 3, GRID, GRID)
    row_index = jnp.arange(GRID)[:, None]
    col_index = jnp.arange(GRID)[None, :]
    offset = jnp.abs(row_index - col_index)
    key_diagonal = jax.random.fold_in(key, 21)
    key_band = jax.random.fold_in(key, 22)
    key_dense = jax.random.fold_in(key, 23)
    diagonal_part = jax.random.uniform(key_diagonal, full_shape, jnp.float32, 0.8, 1.2)
    band_part = jax.random.uniform(key_band, full_shape, jnp.float32, 0.03, 0.25)
    dense_part = jax.random.uniform(key_dense, full_shape, jnp.float32, 0.0, 0.02)
    table = jnp.where(offset == 0, diagonal_part, jnp.where(offset <= 2, band_part, 0.0)) + dense_part
    return table.astype(jnp.bfloat16)


def set_ends(result, stream_key, least, high):
    index_at = [jax.random.randint(jax.random.fold_in(stream_key, axis), (), 0, length) for axis, length in enumerate(result.shape)]
    main_axis = result.shape.index(max(result.shape))
    beside = index_at[:main_axis] + [(index_at[main_axis] + 1) % result.shape[main_axis]] + index_at[main_axis + 1:]
    return result.at[tuple(index_at)].set(least).at[tuple(beside)].set(high)


def setup_inputs(seed: int = 0) -> dict:
    keys = jax.random.split(jax.random.key(seed), 5)
    particles = draw_particles(jax.random.fold_in(keys[4], 71), 0)
    orient_bin = set_ends(jax.random.randint(keys[1], (PARTICLES,), 0, BINS), jax.random.fold_in(keys[1], 1), 0, BINS - 1).astype(jnp.int32)
    tilt_slope = set_ends(jax.random.randint(keys[2], (PARTICLES, 2), 12, 41), jax.random.fold_in(keys[2], 1), 12, 40).astype(jnp.int32)
    interp_table = draw_interp_table(jax.random.fold_in(keys[4], 71), 0)
    return dict(particles=particles, orient_bin=orient_bin, tilt_slope=tilt_slope, interp_table=interp_table)


def wedge_mask(tilt_limits, grid_size):
    centre = grid_size // 2
    wave_first = (jnp.arange(grid_size, dtype=jnp.int32) - centre)[:, None]
    wave_third = (jnp.arange(grid_size * grid_size, dtype=jnp.int32) % grid_size - centre)[None, :]
    tilt_limit = jnp.where(wave_first * wave_third >= 0, tilt_limits[0], tilt_limits[1])
    inside = 16 * jnp.abs(wave_third) <= tilt_limit * jnp.abs(wave_first)
    return inside.astype(jnp.float32)

def interpolate(stacked, kernels, grid_size):
    components = stacked.shape[0]
    kernels = kernels.astype(jnp.float32)
    along_first = jnp.einsum('ax,cxm->cam', kernels[0], stacked.astype(jnp.float32), precision=lax.Precision.HIGHEST).astype(jnp.bfloat16)
    along_first = along_first.reshape(components, grid_size, grid_size, grid_size)
    along_second = jnp.einsum('by,cayz->cabz', kernels[1], along_first.astype(jnp.float32), precision=lax.Precision.HIGHEST).astype(jnp.bfloat16)
    along_third = jnp.einsum('dz,cabz->cabd', kernels[2], along_second.astype(jnp.float32), precision=lax.Precision.HIGHEST)
    return along_third.reshape(components, grid_size, grid_size * grid_size)

def reference(particles, orient_bin, tilt_slope, interp_table):
    grid_size = GRID
    half_labels = (jnp.arange(PARTICLES, dtype=jnp.int32) // (PARTICLES // 2)).astype(jnp.int32)

    def insert_one(partial_value, inputs):
        volume_data, bin_row, tilt_limits, half_label = inputs
        weight = wedge_mask(tilt_limits, grid_size)
        stacked = jnp.stack([volume_data[0] * weight, volume_data[1] * weight, weight]).astype(jnp.bfloat16)
        kernels = interp_table[bin_row]
        inserted = interpolate(stacked, kernels, grid_size)
        partial_value = partial_value.at[half_label].add(inserted)
        return (partial_value, None)
    partial_value = jnp.zeros((2, 3, grid_size, grid_size * grid_size), jnp.float32)
    partial_value, unused_out = lax.scan(insert_one, partial_value, (particles, orient_bin, tilt_slope, half_labels))
    half_maps = partial_value[:, :2] / (partial_value[:, 2:3] + 1.0)
    centre = grid_size // 2
    wave_first = (jnp.arange(grid_size, dtype=jnp.int32) - centre)[:, None]
    plane_index = jnp.arange(grid_size * grid_size, dtype=jnp.int32)[None, :]
    wave_second = plane_index // grid_size - centre
    wave_third = plane_index % grid_size - centre
    radius_sq = (wave_first * wave_first + wave_second * wave_second + wave_third * wave_third).reshape(-1)
    bounds = jnp.arange(4, centre, dtype=jnp.int32)
    shell_index = lax.optimization_barrier(jnp.sum((radius_sq[:, None] >= (bounds * bounds)[None, :]).astype(jnp.int32), axis=1)).astype(jnp.int32)
    shell_index = jnp.where(radius_sq < centre * centre, shell_index, SHELLS).astype(jnp.int32)
    map_first = half_maps[0]
    map_second = half_maps[1]
    cross_term = (map_first[0] * map_second[0] + map_first[1] * map_second[1]).reshape(-1)
    power_first = (map_first[0] * map_first[0] + map_first[1] * map_first[1]).reshape(-1)
    power_second = (map_second[0] * map_second[0] + map_second[1] * map_second[1]).reshape(-1)

    def shell_sum(values):
        return jax.ops.segment_sum(values, shell_index, num_segments=SHELLS + 1)[:SHELLS]
    cross_sum = shell_sum(cross_term)
    first_sum = shell_sum(power_first)
    second_sum = shell_sum(power_second)
    counts = shell_sum(jnp.ones_like(cross_term))
    shell_power = jnp.stack([first_sum, second_sum]) / counts[None, :]
    correlation = cross_sum / jnp.sqrt(first_sum * second_sum + 1e-06)
    shell_correlation = jnp.stack([correlation, correlation])
    return (half_maps, shell_power, shell_correlation)
```

```python
import functools

import jax
import jax.numpy as jnp
from jax import lax
from jax.experimental import pallas as pl
from jax.experimental.pallas import tpu as pltpu
from jax.sharding import Mesh
from jax.sharding import PartitionSpec as P

SHELLS = 29
GRID = 64
BINS = 16
STRIDE = 72
HALF_ROW_COL = ("half", "row_0", "row_1", "col")
MESH = pl.DeviceIdType.MESH
F32 = jnp.float32
BF16 = jnp.bfloat16


def iota(shape, dim):
    return lax.broadcasted_iota(jnp.int32, shape, dim)


def insert_kernel(bin_ref, slope_ref, particle_ref, table_ref, v0_ref, v1_ref, info_ref, mid0_ref, mid1_ref):
    lane = iota((1, 128), 1)
    row = jnp.zeros((1, 128), jnp.int32)
    for particle in range(2):
        row = jnp.where(lane == particle, bin_ref[particle], row)
        for side in range(2):
            row = jnp.where(lane == 2 + 2 * particle + side, slope_ref[particle, side], row)
    info_ref[...] = row

    wave_first = iota((GRID, 128), 0) - 32
    wave_third = (iota((GRID, 128), 1) & 63) - 32
    same_side = wave_first * wave_third >= 0
    block_row = iota((256, 256), 0) // 64
    block_col = iota((256, 256), 1) // 64
    matching = (block_row // 2 == block_col % 2) & (block_row % 2 == block_col // 2)

    for particle, mid_ref in enumerate((mid0_ref, mid1_ref)):
        limit = jnp.where(same_side, slope_ref[particle, 0], slope_ref[particle, 1])
        inside = 16 * jnp.abs(wave_third) <= limit * jnp.abs(wave_first)
        weight = inside.astype(F32).astype(BF16)
        which = bin_ref[particle]
        along_first = table_ref[which, 0]
        third = jnp.transpose(table_ref[which, 2].astype(F32))
        third = jnp.concatenate([third, third], axis=1)
        third = jnp.concatenate([third, third], axis=1)
        third = jnp.concatenate([third, third, third, third], axis=0)
        along_third = jnp.where(matching, third, 0.0).astype(BF16)

        def pairs(step, carry):
            for inner in range(4):
                pair = step * 4 + inner
                columns = pl.ds(pl.multiple_of(pair * 128, 128), 128)
                data = jnp.concatenate(
                    [particle_ref[particle, part, :, columns] * weight for part in range(2)], axis=1
                )
                first = jnp.dot(along_first, data, preferred_element_type=F32).astype(BF16)
                both = jnp.dot(first, along_third, preferred_element_type=F32)
                start = pl.multiple_of(pair * (2 * STRIDE), 8)
                mid_ref[pl.ds(start, GRID), :] = both[:, :128]
                mid_ref[pl.ds(start + STRIDE, GRID), :] = both[:, 128:]
            return carry

        lax.fori_loop(0, 8, pairs, 0)

    along_second = jnp.concatenate(
        [table_ref[bin_ref[particle], 1].astype(F32) for particle in range(2)], axis=1
    ).astype(BF16)

    for slow in range(4):

        def slabs(fast, carry):
            for color, out_ref in enumerate((v0_ref, v1_ref)):
                places = []
                for inner in range(2):
                    first = 16 * slow + 4 * fast + 2 * color + inner
                    if color == 1:
                        first = 16 * fast + 4 * slow + 2 * color + inner
                    rows = [
                        mid_ref[pl.ds(first, GRID, stride=STRIDE), :]
                        for mid_ref in (mid0_ref, mid1_ref)
                    ]
                    places.append(jnp.concatenate(rows, axis=0).astype(BF16))
                slab = jnp.dot(
                    along_second, jnp.concatenate(places, axis=1), preferred_element_type=F32
                )
                out_ref[slow, fast, 0] = slab[:, :128]
                out_ref[slow, fast, 1] = slab[:, 128:]
            return carry

        lax.fori_loop(0, 4, slabs, 0)


def insert(particles, orient_bin, tilt_slope, interp_table):
    smem = pl.BlockSpec(memory_space=pltpu.SMEM)
    vmem = pl.BlockSpec(memory_space=pltpu.VMEM)
    volume = jax.ShapeDtypeStruct((4, 4, 2, GRID, 128), F32)
    return pl.pallas_call(
        insert_kernel,
        out_shape=(volume, volume, jax.ShapeDtypeStruct((1, 128), jnp.int32)),
        in_specs=[smem, smem, vmem, vmem],
        out_specs=(vmem, vmem, vmem),
        scratch_shapes=[pltpu.VMEM((GRID * STRIDE, 128), F32)] * 2,
        compiler_params=pltpu.CompilerParams(vmem_limit_bytes=32 * 2**20),
        name="insert",
    )(orient_bin, tilt_slope, particles, interp_table)


def weight_sums(info, row, col, table_ref, count_ref, first_ref, second_ref):
    lane = iota((128, 128), 1)
    side_lane = lane & 63
    bins, slopes = [], []
    for particle in range(2):
        bins.append((info[:, particle : particle + 1] == lane).astype(F32))
        limit = jnp.where(
            lane < 64, info[:, 2 + 2 * particle : 3 + 2 * particle], info[:, 3 + 2 * particle : 4 + 2 * particle]
        )
        slopes.append((limit == side_lane).astype(F32))
    bins = jnp.concatenate([jnp.transpose(part)[:BINS] for part in bins], axis=1).astype(BF16)
    slopes = jnp.concatenate(slopes, axis=0).astype(BF16)
    histogram = jnp.dot(bins, slopes, preferred_element_type=F32).astype(BF16)

    wave_third = (iota((128, 128), 1) & 63) - 32
    reach = (16 * jnp.abs(wave_third)).astype(F32)
    limit = (iota((128, 128), 0) & 63).astype(F32)
    same_side = iota((128, 128), 0) < 64
    nonneg_third, nonpos_third = wave_third >= 0, wave_third <= 0

    def planes(first, carry):
        wave_first = first - 32
        agree = (
            ((wave_first > 0) & nonneg_third) | ((wave_first < 0) & nonpos_third) | (wave_first == 0)
        )
        inside = (reach <= limit * jnp.abs(wave_first).astype(F32)) & (agree == same_side)
        counts = jnp.dot(histogram, inside.astype(F32).astype(BF16), preferred_element_type=F32)
        count_ref[pl.ds(pl.multiple_of(first * BINS, BINS), BINS), :] = counts
        return carry

    lax.fori_loop(0, GRID, planes, 0)

    bin_lane = iota((GRID, 128), 1)
    second = jnp.zeros((GRID, 128), F32)
    for which in range(BINS):
        counts = count_ref[pl.ds(which, GRID, stride=BINS), :].astype(BF16)
        first_ref[which] = jnp.dot(table_ref[which, 0], counts, preferred_element_type=F32)
        total = jnp.sum(table_ref[which, 1].astype(F32), axis=1, keepdims=True)
        second = jnp.where(bin_lane == which, total, second)
    second_ref[...] = second
    second = second_ref[pl.ds(pl.multiple_of(col * 8, 8), 8), :]
    sums = [jnp.zeros((8, 128), F32) for _ in range(4)]
    for which in range(BINS):
        first = first_ref[which, pl.ds(row * 4, 4), :][:, :GRID]
        high = first.astype(BF16)
        low = (first - high.astype(F32)).astype(BF16)
        third = jnp.concatenate([table_ref[which, 2]] * 2, axis=0)
        contract = functools.partial(
            lax.dot_general, dimension_numbers=(((1,), (1,)), ((), ())), preferred_element_type=F32
        )
        plane = contract(high, third) + contract(low, third)
        for index in range(4):
            sums[index] = sums[index] + second[:, which : which + 1] * plane[index : index + 1]
    return sums


class Ring4:
    def __init__(self, axis, source, buffer, send, recv):
        self.axis, self.source, self.buffer, self.send, self.recv = axis, source, buffer, send, recv
        self.me = lax.axis_index(axis)
        self.right, self.far, self.left = ((self.me + step) % 4 for step in (1, 2, 3))
        self.copies = [None] * 6

    def copy(self, slot, source, target):
        self.copies[slot] = pltpu.make_async_remote_copy(
            src_ref=source,
            dst_ref=self.buffer.at[slot],
            send_sem=self.send.at[slot],
            recv_sem=self.recv.at[slot],
            device_id={self.axis: target},
            device_id_type=MESH,
        )
        self.copies[slot].start()

    def begin(self):
        self.copy(0, self.source(self.far, 0), self.right)
        self.copy(3, self.source(self.far, 1), self.left)
        self.copy(2, self.source(self.right, 1), self.right)
        self.copy(5, self.source(self.left, 0), self.left)

    def forward(self):
        self.copies[0].wait_recv()
        self.buffer[0] = self.buffer[0] + self.source(self.right, 0)[...]
        self.copy(1, self.buffer.at[0], self.right)
        self.copies[3].wait_recv()
        self.buffer[3] = self.buffer[3] + self.source(self.left, 1)[...]
        self.copy(4, self.buffer.at[3], self.left)

    def finish(self, result):
        for half, near, other in ((0, 1, 5), (1, 4, 2)):
            self.copies[other].wait_recv()
            self.copies[near].wait_recv()
            result(half)[...] = self.source(self.me, half)[...] + self.buffer[near] + self.buffer[other]

    def drain(self):
        for copy in self.copies:
            copy.wait_send()


def exchange(axis, size, source, target, send, recv):
    me = lax.axis_index(axis)
    copies = []
    for step in range(1, size):
        peer = (me + step) % size
        copy = pltpu.make_async_remote_copy(
            src_ref=source(peer),
            dst_ref=target,
            send_sem=send.at[step],
            recv_sem=recv.at[step],
            device_id={axis: peer},
            device_id_type=MESH,
        )
        copy.start()
        copies.append(copy)
    return copies


def shell_rows(sums_first, sums_second, row, col):
    wave_second = iota((8, 128), 0) + col * 8 - 32
    wave_third = (iota((8, 128), 1) & 63) - 32
    plane = wave_second * wave_second + wave_third * wave_third
    radius = []
    for index in range(4):
        wave_first = row * 4 + index - 32
        radius.append(plane + wave_first * wave_first)
    real = iota((8, 128), 1) < 64
    values = [
        [first * second for first, second in zip(sums_first, sums_second)],
        [first * first for first in sums_first],
        [second * second for second in sums_second],
        [jnp.where(real, 1.0, 0.0).astype(F32)] * 4,
    ]
    rows = [[] for _ in range(4)]
    for shell in range(32):
        low = 0 if shell == 0 else (shell + 3) ** 2
        high = (shell + 4) ** 2 if shell < SHELLS else low
        masks = [(r >= low) & (r < high) for r in radius]
        for kind in range(4):
            parts = [jnp.where(m, v, 0.0) for m, v in zip(masks, values[kind])]
            total = (parts[0] + parts[1]) + (parts[2] + parts[3])
            rows[kind].append(jnp.sum(total, axis=0, keepdims=True))
    stacked = jnp.concatenate([row for kind in rows for row in kind], axis=0)
    ones = jnp.ones((8, 128), F32)
    return lax.dot_general(
        ones,
        stacked,
        dimension_numbers=(((1,), (1,)), ((), ())),
        precision=lax.Precision.HIGHEST,
        preferred_element_type=F32,
    )[:1]


def reduce_kernel(
    info_ref, table_ref, v0_ref, v1_ref, map_ref, stat_ref,
    ring_a, ring_b, ring_c, ring_d, part0, part1, slab, planes, gathered, own, other, stat_x, stat_y, stat_z,
    count_ref, first_ref, second_ref, ring_send, ring_recv, small_send, small_recv,
):
    half, x, y, z = (lax.axis_index(name) for name in HALF_ROW_COL)
    row = x * 4 + y
    barrier = pltpu.get_barrier_semaphore()
    for axis, size in (("row_0", 4), ("row_1", 4), ("col", 8), ("half", 2)):
        for step in range(1, size):
            peer = (lax.axis_index(axis) + step) % size
            pl.semaphore_signal(barrier, inc=1, device_id={axis: peer}, device_id_type=MESH)
    pl.semaphore_wait(barrier, 14)

    def small(index):
        return small_send.at[index], small_recv.at[index]

    def outer(ref):
        return lambda owner, side: ref.at[owner, pl.ds(2 * side, 2)]

    pending = []
    gathered[z, y, x] = info_ref[...]
    spread = exchange("row_0", 4, lambda peer: info_ref, gathered.at[z, y, x], *small(0))
    pending += spread
    first = [
        Ring4("row_0", outer(v0_ref), ring_a, ring_send.at[0], ring_recv.at[0]),
        Ring4("row_1", outer(v1_ref), ring_b, ring_send.at[1], ring_recv.at[1]),
    ]
    for ring in first:
        ring.begin()
    for copy in spread:
        copy.wait_recv()
    spread = exchange("row_1", 4, lambda peer: gathered.at[z, y], gathered.at[z, y], *small(1))
    pending += spread
    for ring in first:
        ring.forward()
    for copy in spread:
        copy.wait_recv()
    spread = exchange("col", 8, lambda peer: gathered.at[z], gathered.at[z], *small(2))
    pending += spread
    for ring, part in zip(first, (part0, part1)):
        ring.finish(lambda side, part=part: part.at[pl.ds(2 * side, 2)])

    second = [
        Ring4("row_1", lambda owner, side: part0.at[owner, side], ring_c, ring_send.at[2], ring_recv.at[2]),
        Ring4("row_0", lambda owner, side: part1.at[owner, side], ring_d, ring_send.at[3], ring_recv.at[3]),
    ]
    for ring in second:
        ring.begin()
    for copy in spread:
        copy.wait_recv()
    for ring in second:
        ring.forward()
    for color, ring in enumerate(second):
        ring.finish(lambda side, color=color: slab.at[2 * color + side])

    spread = exchange(
        "col", 8, lambda peer: slab.at[:, pl.ds(pl.multiple_of(peer * 8, 8), 8)], planes.at[z], *small(3)
    )
    pending += spread
    weights = weight_sums(
        gathered[...].reshape(128, 128), row, z, table_ref, count_ref, first_ref, second_ref
    )
    for copy in spread:
        copy.wait_recv()
    for index in range(4):
        total = slab[index, pl.ds(pl.multiple_of(z * 8, 8), 8)]
        for step in range(1, 8):
            total = total + planes[(z + step) % 8, index]
        own[index] = total / (weights[index] + 1.0)
    partner = exchange("half", 2, lambda peer: own, other, *small(4))
    pending += partner
    map_ref[...] = own[...]
    partner[0].wait_recv()
    on_first = half == 0
    mine = [own[index] for index in range(4)]
    theirs = [other[index] for index in range(4)]
    maps_first = [jnp.where(on_first, a, b) for a, b in zip(mine, theirs)]
    maps_second = [jnp.where(on_first, b, a) for a, b in zip(mine, theirs)]
    stat = shell_rows(maps_first, maps_second, row, z)
    for number, (axis, size, ref) in enumerate((("row_0", 4, stat_x), ("row_1", 4, stat_y), ("col", 8, stat_z))):
        me = lax.axis_index(axis)
        ref[me] = stat
        spread = exchange(axis, size, lambda peer: ref.at[me], ref.at[me], *small(5 + number))
        pending += spread
        for copy in spread:
            copy.wait_recv()
        stat = ref[0]
        for index in range(1, size):
            stat = stat + ref[index]
    stat_ref[...] = stat
    for ring in first + second:
        ring.drain()
    for copy in pending:
        copy.wait_send()


def reduce_maps(info, interp_table, v0, v1):
    vmem = pl.BlockSpec(memory_space=pltpu.VMEM)
    big, little = pltpu.VMEM((6, 2, 2, GRID, 128), F32), pltpu.VMEM((6, GRID, 128), F32)
    stat = lambda size: pltpu.VMEM((size, 1, 128), F32)
    return pl.pallas_call(
        reduce_kernel,
        out_shape=(jax.ShapeDtypeStruct((4, 8, 128), F32), jax.ShapeDtypeStruct((1, 128), F32)),
        in_specs=[vmem] * 4,
        out_specs=(vmem, vmem),
        scratch_shapes=[
            big,
            big,
            little,
            little,
            pltpu.VMEM((4, 2, GRID, 128), F32),
            pltpu.VMEM((4, 2, GRID, 128), F32),
            pltpu.VMEM((4, GRID, 128), F32),
            pltpu.VMEM((8, 4, 8, 128), F32),
            pltpu.VMEM((8, 4, 4, 1, 128), jnp.int32),
            pltpu.VMEM((4, 8, 128), F32),
            pltpu.VMEM((4, 8, 128), F32),
            stat(4),
            stat(4),
            stat(8),
            pltpu.VMEM((GRID * BINS, 128), F32),
            pltpu.VMEM((BINS, GRID, 128), F32),
            pltpu.VMEM((GRID, 128), F32),
            pltpu.SemaphoreType.DMA((4, 6)),
            pltpu.SemaphoreType.DMA((4, 6)),
            pltpu.SemaphoreType.DMA((8, 8)),
            pltpu.SemaphoreType.DMA((8, 8)),
        ],
        compiler_params=pltpu.CompilerParams(
            collective_id=0, has_side_effects=True, vmem_limit_bytes=32 * 2**20
        ),
        name="reduce",
    )(info, interp_table, v0, v1)


def local(particles, orient_bin, tilt_slope, interp_table):
    v0, v1, info = insert(particles, orient_bin, tilt_slope, interp_table)
    maps, stat = reduce_maps(info, interp_table, v0, v1)
    half_maps = maps.reshape(4, 8, 2, GRID).transpose(2, 0, 1, 3).reshape(1, 2, 4, 8 * GRID)
    cross, power_first, power_second, counts = (
        stat[0, 32 * kind : 32 * kind + SHELLS] for kind in range(4)
    )
    shell_power = jnp.stack([power_first, power_second]) / counts[None, :]
    shell_correlation = (cross / jnp.sqrt(power_first * power_second + 1e-06))[None]
    return half_maps, shell_power, shell_correlation


def solution(mesh):
    torus = Mesh(
        mesh.devices.reshape(mesh.shape["half"], 4, 4, mesh.shape["col"]), HALF_ROW_COL
    )
    in_specs = (P(HALF_ROW_COL, None, None, None), P(HALF_ROW_COL), P(HALF_ROW_COL, None), P())
    out_specs = (P("half", None, ("row_0", "row_1"), "col"), P(), P("half", None))
    return jax.shard_map(local, mesh=torus, in_specs=in_specs, out_specs=out_specs, check_vma=False)
```

```python
import functools

import jax
import jax.numpy as jnp
from jax import lax
from jax.experimental import pallas as pl
from jax.experimental.pallas import tpu as pltpu
from jax.sharding import Mesh
from jax.sharding import PartitionSpec as P

SHELLS = 29
GRID = 64
BINS = 16
STRIDE = 24
HALF_ROW_COL = ("half", "row_0", "row_1", "col")
MESH = pl.DeviceIdType.MESH
F32 = jnp.float32
BF16 = jnp.bfloat16


def iota(shape, dim):
    return lax.broadcasted_iota(jnp.int32, shape, dim)


def owner_rows(x, y):
    index = iota((GRID, GRID), 0)
    group, color, other, inner = index // 16, (index // 8) % 2, (index // 2) % 4, index % 2
    shift = jnp.where(group == 0, 2, jnp.where(group == 1, 1, jnp.where(group == 2, 3, 0)))
    main = (jnp.where(color == 0, x, y) + shift) % 4
    plane = jnp.where(color == 0, 16 * main + 4 * other, 16 * other + 4 * main + 2) + inner
    return (plane == iota((GRID, GRID), 1)).astype(F32).astype(BF16)


def along_first(particle, order, bins, slopes, data, table, first):
    wave_first = iota((GRID, 128), 0) - 32
    wave_third = (iota((GRID, 128), 1) & 63) - 32
    limit = jnp.where(wave_first * wave_third >= 0, slopes[particle, 0], slopes[particle, 1])
    inside = 16 * jnp.abs(wave_third) <= limit * jnp.abs(wave_first)
    weight = inside.astype(F32).astype(BF16)
    kernel = jnp.dot(order, table[bins[particle], 0], preferred_element_type=F32).astype(BF16)

    def pairs(step, carry):
        for inner in range(16):
            pair = step * 16 + inner
            columns = pl.ds(pl.multiple_of(pair * 128, 128), 128)
            both = jnp.concatenate([data[particle, part, :, columns] * weight for part in range(2)], axis=1)
            first[particle, pair] = jnp.dot(kernel, both, preferred_element_type=F32).astype(BF16)
        return carry

    lax.fori_loop(0, 2, pairs, 0)


def third_operator(kernel):
    block_row = iota((256, 256), 0) // 64
    block_col = iota((256, 256), 1) // 64
    matching = (block_row // 2 == block_col % 2) & (block_row % 2 == block_col // 2)
    third = jnp.transpose(kernel.astype(F32))
    third = jnp.concatenate([third, third], axis=1)
    third = jnp.concatenate([third, third], axis=1)
    third = jnp.concatenate([third, third, third, third], axis=0)
    return jnp.where(matching, third, 0.0).astype(BF16)


def insert_group(group, operators, second, first, middles, volume):
    rows = pl.ds(16 * group, 16)
    for particle, middle in enumerate(middles):
        lines = first[particle, :, rows, :].reshape(512, 256)
        lines = jnp.dot(lines, operators[particle], preferred_element_type=F32)
        for pair in range(32):
            middle[pl.ds(2 * pair * STRIDE, 16), :] = lines[16 * pair : 16 * pair + 16, :128]
            middle[pl.ds((2 * pair + 1) * STRIDE, 16), :] = lines[16 * pair : 16 * pair + 16, 128:]
    for place in range(8):
        planes = []
        for inner in range(2):
            sides = [middle[pl.ds(2 * place + inner, GRID, stride=STRIDE), :] for middle in middles]
            planes.append(jnp.concatenate(sides, axis=0).astype(BF16))
        slab = jnp.dot(second, jnp.concatenate(planes, axis=1), preferred_element_type=F32)
        for inner in range(2):
            volume[group, place // 4, inner, place % 4] = slab[:, 128 * inner : 128 * inner + 128]


def bin_counts(infos, count_ref):
    lane = iota((128, 128), 1)
    histograms = []
    for info in infos:
        bins, slopes = [], []
        for particle in range(2):
            bins.append((info[:, particle : particle + 1] == lane).astype(F32))
            limit = jnp.where(
                lane < 64,
                info[:, 2 + 2 * particle : 3 + 2 * particle],
                info[:, 3 + 2 * particle : 4 + 2 * particle],
            )
            slopes.append((limit == (lane & 63)).astype(F32))
        bins = jnp.concatenate([jnp.transpose(part)[:BINS] for part in bins], axis=1).astype(BF16)
        slopes = jnp.concatenate(slopes, axis=0).astype(BF16)
        histograms.append(jnp.dot(bins, slopes, preferred_element_type=F32))
    histogram = jnp.concatenate(histograms, axis=0).astype(BF16)

    wave_third = (iota((128, 128), 1) & 63) - 32
    reach = (16 * jnp.abs(wave_third)).astype(F32)
    limit = (iota((128, 128), 0) & 63).astype(F32)
    same_side = iota((128, 128), 0) < 64
    nonneg_third, nonpos_third = wave_third >= 0, wave_third <= 0

    def planes(step, carry):
        for inner in range(4):
            first = step * 4 + inner
            wave_first = first - 32
            agree = (
                ((wave_first > 0) & nonneg_third) | ((wave_first < 0) & nonpos_third) | (wave_first == 0)
            )
            inside = (reach <= limit * jnp.abs(wave_first).astype(F32)) & (agree == same_side)
            counts = jnp.dot(histogram, inside.astype(F32).astype(BF16), preferred_element_type=F32)
            count_ref[pl.ds(pl.multiple_of(first * 2 * BINS, 2 * BINS), 2 * BINS), :] = counts
        return carry

    lax.fori_loop(0, GRID // 4, planes, 0)


def insert_counts(table, count_ref, first_ref, second_ref):
    bin_lane = iota((GRID, 128), 1)
    second = jnp.zeros((GRID, 128), F32)
    for which in range(BINS):
        counts = [count_ref[pl.ds(BINS * half + which, GRID, stride=2 * BINS), :] for half in range(2)]
        counts = jnp.concatenate(counts, axis=1).astype(BF16)
        lines = jnp.dot(table[which, 0], counts, preferred_element_type=F32)
        for half in range(2):
            first_ref[half, which] = lines[:, 128 * half : 128 * half + 128]
        total = jnp.sum(table[which, 1].astype(F32), axis=1, keepdims=True)
        second = jnp.where(bin_lane == which, total, second)
    second_ref[...] = second


def weight_sums(plane, col, table, first_ref, second_ref, weight_ref):
    second = second_ref[pl.ds(pl.multiple_of(col * 8, 8), 8), :]
    contract = functools.partial(
        lax.dot_general, dimension_numbers=(((1,), (1,)), ((), ())), preferred_element_type=F32
    )
    sums = [jnp.zeros((8, 128), F32) for _ in range(4)]
    for which in range(BINS):
        first = jnp.concatenate([first_ref[half, which, pl.ds(plane, 2), :] for half in range(2)], axis=0)[:, :GRID]
        high = first.astype(BF16)
        low = (first - high.astype(F32)).astype(BF16)
        third = jnp.concatenate([table[which, 2]] * 2, axis=0)
        lines = contract(high, third) + contract(low, third)
        for index in range(4):
            sums[index] = sums[index] + second[:, which : which + 1] * lines[index : index + 1]
    for index in range(4):
        weight_ref[index // 2, index % 2] = sums[index]


def remote(source, target, send, recv, device):
    copy = pltpu.make_async_remote_copy(
        src_ref=source, dst_ref=target, send_sem=send, recv_sem=recv, device_id=device, device_id_type=MESH
    )
    copy.start()
    return copy


class Ring4:
    def __init__(self, axis, source, buffer, send, recv):
        self.axis, self.source, self.buffer, self.send, self.recv = axis, source, buffer, send, recv
        me = lax.axis_index(axis)
        self.right, self.left = (me + 1) % 4, (me + 3) % 4
        self.copies = [None] * 6

    def copy(self, slot, source, target):
        self.copies[slot] = remote(
            source, self.buffer.at[slot], self.send.at[slot], self.recv.at[slot], {self.axis: target}
        )

    def send_far(self):
        self.copy(0, self.source(0, 0), self.right)
        self.copy(3, self.source(0, 1), self.left)

    def send_right(self):
        self.copy(2, self.source(1, 1), self.right)

    def send_left(self):
        self.copy(5, self.source(2, 0), self.left)

    def forward(self):
        self.copies[0].wait_recv()
        self.buffer[0] = self.buffer[0] + self.source(1, 0)[...]
        self.copy(1, self.buffer.at[0], self.right)
        self.copies[3].wait_recv()
        self.buffer[3] = self.buffer[3] + self.source(2, 1)[...]
        self.copy(4, self.buffer.at[3], self.left)

    def finish(self, result):
        for half, near, other in ((0, 1, 5), (1, 4, 2)):
            self.copies[other].wait_recv()
            self.copies[near].wait_recv()
            result[pl.ds(2 * half, 2)] = (
                self.source(3, half)[...] + self.buffer[near] + self.buffer[other]
            )


def exchange(me, size, place, source, target, send, recv):
    copies = []
    for step in range(1, size):
        peer = (me + step) % size
        copies.append(remote(source(peer), target, send.at[step], recv.at[step], place(peer)))
    return copies


def arrived(copies):
    for copy in copies:
        copy.wait_recv()


def shell_rows(sums_first, sums_second, plane, col):
    wave_second = iota((8, 128), 0) + col * 8 - 32
    wave_third = (iota((8, 128), 1) & 63) - 32
    rest = wave_second * wave_second + wave_third * wave_third
    radius = []
    for index in range(2):
        wave_first = plane + index - 32
        radius.append(rest + wave_first * wave_first)
    real = iota((8, 128), 1) < 64
    values = [
        [first * second for first, second in zip(sums_first, sums_second)],
        [first * first for first in sums_first],
        [second * second for second in sums_second],
        [jnp.where(real, 1.0, 0.0).astype(F32)] * 2,
    ]
    rows = [[] for _ in range(4)]
    for shell in range(32):
        low = 0 if shell == 0 else (shell + 3) ** 2
        high = (shell + 4) ** 2 if shell < SHELLS else low
        masks = [(r >= low) & (r < high) for r in radius]
        for kind in range(4):
            parts = [jnp.where(m, v, 0.0) for m, v in zip(masks, values[kind])]
            rows[kind].append(jnp.sum(parts[0] + parts[1], axis=0, keepdims=True))
    stacked = jnp.concatenate([row for kind in rows for row in kind], axis=0)
    return lax.dot_general(
        jnp.ones((8, 128), F32),
        stacked,
        dimension_numbers=(((1,), (1,)), ((), ())),
        precision=lax.Precision.HIGHEST,
        preferred_element_type=F32,
    )[:1]


def kernel(
    particle_hbm, bin_hbm, slope_hbm, table_hbm, map_ref, power_ref, correlation_ref,
    data, bins, slopes, table, first, middle0, middle1, volume,
    ring_buffer, part, spread_buffer, slab, planes, info_ref, gathered, weight_ref, own, other, swap, stat_plane, stat_line,
    count_ref, first_ref, second_ref,
    local_sem, ring_send, ring_recv, spread_send, spread_recv, plane_send, plane_recv, small_send, small_recv,
):
    half, x, y, z = (lax.axis_index(name) for name in HALF_ROW_COL)
    in_plane, in_line = x * 4 + y, z * 2 + half
    place_plane = lambda peer: {"row_0": peer // 4, "row_1": peer % 4}
    place_line = lambda peer: {"col": peer // 2, "half": peer % 2}

    barrier = pltpu.get_barrier_semaphore()
    for me, place in ((in_plane, place_plane), (in_line, place_line)):
        for step in range(1, 16):
            pl.semaphore_signal(barrier, inc=1, device_id=place((me + step) % 16), device_id_type=MESH)
    loads = [
        pltpu.make_async_copy(source, target, local_sem.at[index])
        for index, (source, target) in enumerate(
            (
                (bin_hbm, bins),
                (slope_hbm, slopes),
                (table_hbm, table),
                (particle_hbm.at[0], data.at[0]),
                (particle_hbm.at[1], data.at[1]),
            )
        )
    ]
    for load in loads:
        load.start()
    loads[0].wait()
    loads[1].wait()
    lane = iota((1, 128), 1)
    info = jnp.zeros((1, 128), jnp.int32)
    for particle in range(2):
        info = jnp.where(lane == particle, bins[particle], info)
        for side in range(2):
            info = jnp.where(lane == 2 + 2 * particle + side, slopes[particle, side], info)
    info_ref[...] = info

    order = owner_rows(x, y)
    loads[2].wait()
    operators = [third_operator(table[bins[particle], 2]) for particle in range(2)]
    second = jnp.concatenate(
        [table[bins[particle], 1].astype(F32) for particle in range(2)], axis=1
    ).astype(BF16)
    for particle in range(2):
        loads[3 + particle].wait()
        along_first(particle, order, bins, slopes, data, table, first)

    pl.semaphore_wait(barrier, 30)
    gathered[half, z, in_plane] = info_ref[...]
    pending = exchange(
        in_plane, 16, place_plane, lambda peer: info_ref, gathered.at[half, z, in_plane], small_send.at[0], small_recv.at[0]
    )
    info_copies = list(pending)

    rings = [
        [
            Ring4(
                axis,
                lambda group, side, color=color, inner=inner: volume.at[group, color, inner, pl.ds(2 * side, 2)],
                ring_buffer.at[color, inner],
                ring_send.at[color, inner],
                ring_recv.at[color, inner],
            )
            for color, axis in enumerate(("row_0", "row_1"))
        ]
        for inner in range(2)
    ]
    flat = rings[0] + rings[1]
    group = functools.partial(
        insert_group,
        operators=operators, second=second, first=first, middles=(middle0, middle1), volume=volume,
    )
    group(0)
    for ring in flat:
        ring.send_far()
    group(1)
    for ring in flat:
        ring.send_right()
    group(2)
    for ring in flat:
        ring.send_left()
    arrived(info_copies)
    info_copies = exchange(
        in_line, 16, place_line, lambda peer: gathered.at[half, z], gathered.at[half, z], small_send.at[1], small_recv.at[1]
    )
    pending += info_copies
    group(3)
    for ring in rings[0]:
        ring.forward()
    arrived(info_copies)
    bin_counts([gathered[index].reshape(128, 128) for index in range(2)], count_ref)
    for ring in rings[1]:
        ring.forward()
    insert_counts(table, count_ref, first_ref, second_ref)

    own_plane = in_plane * 4 + half * 2
    spreads = []
    for inner in range(2):
        spreads.append([])
        for color, axis in enumerate(("row_1", "row_0")):
            rings[inner][color].finish(part.at[color, inner])
            me = lax.axis_index(axis)
            spreads[inner] += exchange(
                me,
                4,
                lambda peer, axis=axis: {axis: peer},
                lambda peer, color=color, inner=inner: part.at[color, inner, peer],
                spread_buffer.at[color, inner, me],
                spread_send.at[color, inner],
                spread_recv.at[color, inner],
            )
        if inner == 0:
            weight_sums(own_plane, z, table, first_ref, second_ref, weight_ref)
    plane_copies = []
    for inner in range(2):
        arrived(spreads[inner])
        pending += spreads[inner]
        for color, axis in enumerate(("row_1", "row_0")):
            me = lax.axis_index(axis)
            total = part[color, inner, me]
            for step in range(1, 4):
                total = total + spread_buffer[color, inner, (me + step) % 4]
            slab[color, inner] = total
        for core in range(2):
            for step in range(1 - core, 8):
                peer = (z + step) % 8
                target = half if core == 0 else 1 - half
                plane_copies.append(
                    remote(
                        slab.at[target, inner, pl.ds(pl.multiple_of(peer * 8, 8), 8)],
                        planes.at[half, inner, z],
                        plane_send.at[inner, core, step],
                        plane_recv.at[inner, core, step],
                        {"col": peer, "half": target},
                    )
                )
        planes[half, inner, z] = slab[half, inner, pl.ds(pl.multiple_of(z * 8, 8), 8)]
    arrived(plane_copies)
    pending += plane_copies

    maps = [[], []]
    for which in range(2):
        for inner in range(2):
            total = planes[which, inner, 0]
            for index in range(1, 8):
                total = total + planes[which, inner, index]
            maps[which].append(total / (weight_ref[which, inner] + 1.0))
            own[which, inner] = maps[which][inner]
    partner = remote(
        own.at[1 - half], other, small_send.at[4, 0], small_recv.at[4, 0], {"half": 1 - half}
    )
    stat_plane[in_plane] = shell_rows(maps[0], maps[1], own_plane, z)
    copies = exchange(
        in_plane, 16, place_plane, lambda peer: stat_plane.at[in_plane], stat_plane.at[in_plane], small_send.at[2], small_recv.at[2]
    )
    pending += copies
    partner.wait_recv()
    for inner in range(2):
        swap[half * 2 + inner] = own[half, inner]
        swap[(1 - half) * 2 + inner] = other[inner]
    low = iota((4, 128), 1) < 64
    for plane in range(4):
        even = swap[plane, pl.ds(0, 4, stride=2), :]
        odd = swap[plane, pl.ds(1, 4, stride=2), :]
        parts = (
            jnp.where(low, even, pltpu.roll(odd, 64, 1)),
            jnp.where(low, pltpu.roll(even, 64, 1), odd),
        )
        for component in range(2):
            for piece in range(4):
                map_ref[0, component, pl.ds(plane, 1), pl.ds(128 * piece, 128)] = parts[component][
                    piece : piece + 1
                ]
    arrived(copies)

    def summed(ref):
        total = ref[0]
        for index in range(1, 16):
            total = total + ref[index]
        return total

    stat_line[in_line] = summed(stat_plane)
    copies = exchange(
        in_line, 16, place_line, lambda peer: stat_line.at[in_line], stat_line.at[in_line], small_send.at[3], small_recv.at[3]
    )
    pending += copies
    arrived(copies)
    stat = jnp.broadcast_to(summed(stat_line), (8, 128))
    power_first, power_second, counts = (pltpu.roll(stat, 128 - 32 * kind, 1) for kind in (1, 2, 3))
    correlation = stat / jnp.sqrt(power_first * power_second + 1e-06)
    power_ref[pl.ds(0, 1), :] = (power_first / counts)[:1, :SHELLS]
    power_ref[pl.ds(1, 1), :] = (power_second / counts)[:1, :SHELLS]
    correlation_ref[...] = correlation[:1, :SHELLS]
    for ring in flat:
        pending += ring.copies
    pending.append(partner)
    for copy in pending:
        copy.wait_send()


def local(particles, orient_bin, tilt_slope, interp_table):
    hbm = pl.BlockSpec(memory_space=pltpu.HBM)
    vmem = pl.BlockSpec(memory_space=pltpu.VMEM)
    dma = pltpu.SemaphoreType.DMA
    f32 = lambda *shape: pltpu.VMEM(shape, F32)
    return pl.pallas_call(
        kernel,
        out_shape=(
            jax.ShapeDtypeStruct((1, 2, 4, 512), F32),
            jax.ShapeDtypeStruct((2, SHELLS), F32),
            jax.ShapeDtypeStruct((1, SHELLS), F32),
        ),
        in_specs=[hbm] * 4,
        out_specs=(vmem, vmem, vmem),
        scratch_shapes=[
            pltpu.VMEM((2, 2, GRID, GRID * GRID), BF16),
            pltpu.SMEM((2,), jnp.int32),
            pltpu.SMEM((2, 2), jnp.int32),
            pltpu.VMEM((BINS, 3, GRID, GRID), BF16),
            pltpu.VMEM((2, 32, GRID, 256), BF16),
            f32(GRID * STRIDE, 128),
            f32(GRID * STRIDE, 128),
            f32(4, 2, 2, 4, GRID, 128),
            f32(2, 2, 6, 2, GRID, 128),
            f32(2, 2, 4, GRID, 128),
            f32(2, 2, 4, GRID, 128),
            f32(2, 2, GRID, 128),
            f32(2, 2, 8, 8, 128),
            pltpu.VMEM((1, 128), jnp.int32),
            pltpu.VMEM((2, 8, 16, 1, 128), jnp.int32),
            f32(2, 2, 8, 128),
            f32(2, 2, 8, 128),
            f32(2, 8, 128),
            f32(4, 8, 128),
            f32(16, 1, 128),
            f32(16, 1, 128),
            f32(GRID * 2 * BINS, 128),
            f32(2, BINS, GRID, 128),
            f32(GRID, 128),
            dma((5,)),
            dma((2, 2, 6)),
            dma((2, 2, 6)),
            dma((2, 2, 4)),
            dma((2, 2, 4)),
            dma((2, 2, 8)),
            dma((2, 2, 8)),
            dma((5, 16)),
            dma((5, 16)),
        ],
        compiler_params=pltpu.CompilerParams(
            collective_id=0, has_side_effects=True, vmem_limit_bytes=60 * 2**20
        ),
        name="halfmaps",
    )(particles, orient_bin, tilt_slope, interp_table)


def solution(mesh):
    torus = Mesh(
        mesh.devices.reshape(mesh.shape["half"], 4, 4, mesh.shape["col"]), HALF_ROW_COL
    )
    in_specs = (P(HALF_ROW_COL, None, None, None), P(HALF_ROW_COL), P(HALF_ROW_COL, None), P())
    out_specs = (P("half", None, ("row_0", "row_1"), "col"), P(), P("half", None))
    return jax.shard_map(local, mesh=torus, in_specs=in_specs, out_specs=out_specs, check_vma=False)
```

```python
import functools
import itertools

import jax
import jax.numpy as jnp
from jax import lax
from jax.experimental import pallas as pl
from jax.experimental.pallas import tpu as pltpu
from jax.sharding import Mesh
from jax.sharding import PartitionSpec as P

SHELLS = 29
GRID = 64
BINS = 16
STRIDE = 24
SIZES = {"half": 2, "row_0": 4, "row_1": 4, "col": 8}
HALF_ROW_COL = ("half", "row_0", "row_1", "col")
MESH = pl.DeviceIdType.MESH
F32 = jnp.float32
BF16 = jnp.bfloat16


def iota(shape, dim):
    return lax.broadcasted_iota(jnp.int32, shape, dim)


def owner_rows(x, y):
    index = iota((GRID, GRID), 0)
    group, color, other, inner = index // 16, (index // 8) % 2, (index // 2) % 4, index % 2
    shift = jnp.where(group == 0, 2, jnp.where(group == 1, 1, jnp.where(group == 2, 3, 0)))
    main = (jnp.where(color == 0, x, y) + shift) % 4
    plane = jnp.where(color == 0, 16 * main + 4 * other, 16 * other + 4 * main + 2) + inner
    return (plane == iota((GRID, GRID), 1)).astype(F32).astype(BF16)


def along_first(particle, order, bins, slopes, data, table, first):
    wave_first = iota((GRID, 128), 0) - 32
    wave_third = (iota((GRID, 128), 1) & 63) - 32
    limit = jnp.where(wave_first * wave_third >= 0, slopes[particle, 0], slopes[particle, 1])
    inside = 16 * jnp.abs(wave_third) <= limit * jnp.abs(wave_first)
    weight = inside.astype(F32).astype(BF16)
    kernel = jnp.dot(order, table[bins[particle], 0], preferred_element_type=F32).astype(BF16)

    def pairs(step, carry):
        for inner in range(16):
            pair = step * 16 + inner
            columns = pl.ds(pl.multiple_of(pair * 128, 128), 128)
            both = jnp.concatenate([data[particle, part, :, columns] * weight for part in range(2)], axis=1)
            first[particle, pair] = jnp.dot(kernel, both, preferred_element_type=F32).astype(BF16)
        return carry

    lax.fori_loop(0, 2, pairs, 0)


def third_operator(kernel):
    block_row = iota((256, 256), 0) // 64
    block_col = iota((256, 256), 1) // 64
    matching = (block_row // 2 == block_col % 2) & (block_row % 2 == block_col // 2)
    third = jnp.transpose(kernel.astype(F32))
    third = jnp.concatenate([third, third], axis=1)
    third = jnp.concatenate([third, third], axis=1)
    third = jnp.concatenate([third, third, third, third], axis=0)
    return jnp.where(matching, third, 0.0).astype(BF16)


def insert_group(group, operators, second, first, middles, volume):
    rows = pl.ds(16 * group, 16)
    for particle, middle in enumerate(middles):
        lines = first[particle, :, rows, :].reshape(512, 256)
        lines = jnp.dot(lines, operators[particle], preferred_element_type=F32)
        for pair in range(32):
            middle[pl.ds(2 * pair * STRIDE, 16), :] = lines[16 * pair : 16 * pair + 16, :128]
            middle[pl.ds((2 * pair + 1) * STRIDE, 16), :] = lines[16 * pair : 16 * pair + 16, 128:]
    for place in range(8):
        planes = []
        for inner in range(2):
            sides = [middle[pl.ds(2 * place + inner, GRID, stride=STRIDE), :] for middle in middles]
            planes.append(jnp.concatenate(sides, axis=0).astype(BF16))
        slab = jnp.dot(second, jnp.concatenate(planes, axis=1), preferred_element_type=F32)
        for inner in range(2):
            volume[group, place // 4, inner, place % 4] = slab[:, 128 * inner : 128 * inner + 128]


def bin_counts(infos, count_ref):
    contract = functools.partial(
        lax.dot_general, dimension_numbers=(((1,), (1,)), ((), ())), preferred_element_type=F32
    )
    bin_index = iota((BINS, 128), 0).astype(F32)
    slope_index = iota((GRID, 128), 0).astype(F32)
    parts = [[], []]
    for info in infos:
        fields = jnp.transpose(info.astype(F32))[:8]
        bins = [(fields[particle : particle + 1] == bin_index).astype(F32) for particle in range(2)]
        bins = jnp.concatenate(bins, axis=1).astype(BF16)
        for side in range(2):
            slopes = [
                (fields[2 + 2 * particle + side : 3 + 2 * particle + side] == slope_index).astype(F32)
                for particle in range(2)
            ]
            parts[side].append(contract(bins, jnp.concatenate(slopes, axis=1).astype(BF16)))
    histogram = jnp.concatenate(parts[0] + parts[1], axis=0).astype(BF16)

    reach = (16 * jnp.abs((iota((GRID, 128), 1) & 63) - 32)).astype(F32)
    wave_third = (iota((2 * BINS, 128), 1) & 63) - 32
    nonneg, nonpos = wave_third >= 0, wave_third <= 0

    def counted(distance):
        inside = (reach <= slope_index * distance).astype(F32).astype(BF16)
        counts = jnp.dot(histogram, inside, preferred_element_type=F32)
        return counts[: 2 * BINS], counts[2 * BINS :]

    def place(first):
        return pl.ds(pl.multiple_of(first * 2 * BINS, 2 * BINS), 2 * BINS)

    def planes(step, carry):
        for inner in range(8):
            distance = step * 8 + inner + 1
            same, opposite = counted(distance.astype(F32))
            count_ref[place(32 + distance), :] = jnp.where(nonneg, same, opposite)
            count_ref[place(32 - distance), :] = jnp.where(nonpos, same, opposite)
        return carry

    count_ref[place(32), :] = counted(0.0)[0]
    lax.fori_loop(0, 4, planes, 0)


def insert_counts(table, count_ref, first_ref, second_ref):
    bin_lane = iota((GRID, 128), 1)
    second = jnp.zeros((GRID, 128), F32)
    for which in range(BINS):
        counts = [count_ref[pl.ds(BINS * half + which, GRID, stride=2 * BINS), :] for half in range(2)]
        counts = jnp.concatenate(counts, axis=1).astype(BF16)
        lines = jnp.dot(table[which, 0], counts, preferred_element_type=F32)
        for half in range(2):
            first_ref[half, which] = lines[:, 128 * half : 128 * half + 128]
        total = jnp.sum(table[which, 1].astype(F32), axis=1, keepdims=True)
        second = jnp.where(bin_lane == which, total, second)
    second_ref[...] = second


def weight_sums(plane, col, table, first_ref, second_ref, weight_ref):
    second = second_ref[pl.ds(pl.multiple_of(col * 8, 8), 8), :]
    contract = functools.partial(
        lax.dot_general, dimension_numbers=(((1,), (1,)), ((), ())), preferred_element_type=F32
    )
    sums = [jnp.zeros((8, 128), F32) for _ in range(4)]
    for which in range(BINS):
        first = jnp.concatenate([first_ref[half, which, pl.ds(plane, 2), :] for half in range(2)], axis=0)[:, :GRID]
        high = first.astype(BF16)
        low = (first - high.astype(F32)).astype(BF16)
        third = jnp.concatenate([table[which, 2]] * 2, axis=0)
        lines = contract(high, third) + contract(low, third)
        for index in range(4):
            sums[index] = sums[index] + second[:, which : which + 1] * lines[index : index + 1]
    for index in range(4):
        weight_ref[index // 2, index % 2] = sums[index]


def remote(source, target, send, recv, device):
    copy = pltpu.make_async_remote_copy(
        src_ref=source, dst_ref=target, send_sem=send, recv_sem=recv, device_id=device, device_id_type=MESH
    )
    copy.start()
    return copy


class Ring4:
    def __init__(self, axis, source, buffer, send, recv):
        self.axis, self.source, self.buffer, self.send, self.recv = axis, source, buffer, send, recv
        me = lax.axis_index(axis)
        self.right, self.left = (me + 1) % 4, (me + 3) % 4
        self.copies = [None] * 6

    def copy(self, slot, source, target):
        self.copies[slot] = remote(
            source, self.buffer.at[slot], self.send.at[slot], self.recv.at[slot], {self.axis: target}
        )

    def send_far(self):
        self.copy(0, self.source(0, 0), self.right)
        self.copy(3, self.source(0, 1), self.left)

    def send_right(self):
        self.copy(2, self.source(1, 1), self.right)

    def send_left(self):
        self.copy(5, self.source(2, 0), self.left)

    def forward(self):
        self.copies[0].wait_recv()
        self.buffer[0] = self.buffer[0] + self.source(1, 0)[...]
        self.copy(1, self.buffer.at[0], self.right)
        self.copies[3].wait_recv()
        self.buffer[3] = self.buffer[3] + self.source(2, 1)[...]
        self.copy(4, self.buffer.at[3], self.left)

    def finish(self, result):
        for half, near, other in ((0, 1, 5), (1, 4, 2)):
            self.copies[other].wait_recv()
            self.copies[near].wait_recv()
            result[pl.ds(2 * half, 2)] = (
                self.source(3, half)[...] + self.buffer[near] + self.buffer[other]
            )


def hops(offset, sizes):
    return sum(min(step, size - step) for step, size in zip(offset, sizes))


def others(*axes):
    sizes = [SIZES[axis] for axis in axes]
    offsets = [offset for offset in itertools.product(*map(range, sizes)) if any(offset)]
    offsets.sort(key=lambda offset: -hops(offset, sizes))
    places = {
        axis: [lax.rem(lax.axis_index(axis) + step, size) for step in range(size)]
        for axis, size in zip(axes, sizes)
    }
    return [{axis: places[axis][step] for axis, step in zip(axes, offset)} for offset in offsets]


def exchange(peers, source, target, send, recv):
    return [
        remote(source(peer), target, send.at[index], recv.at[index], peer) for index, peer in enumerate(peers)
    ]


def arrived(copies):
    for copy in copies:
        copy.wait_recv()


def shell_rows(sums_first, sums_second, plane, col):
    wave_second = iota((8, 128), 0) + col * 8 - 32
    wave_third = (iota((8, 128), 1) & 63) - 32
    rest = wave_second * wave_second + wave_third * wave_third
    radius = []
    for index in range(2):
        wave_first = plane + index - 32
        radius.append(rest + wave_first * wave_first)
    real = iota((8, 128), 1) < 64
    values = [
        [first * second for first, second in zip(sums_first, sums_second)],
        [first * first for first in sums_first],
        [second * second for second in sums_second],
        [jnp.where(real, 1.0, 0.0).astype(F32)] * 2,
    ]
    rows = [[] for _ in range(4)]
    for shell in range(32):
        low = 0 if shell == 0 else (shell + 3) ** 2
        high = (shell + 4) ** 2 if shell < SHELLS else low
        masks = [(r >= low) & (r < high) for r in radius]
        for kind in range(4):
            parts = [jnp.where(m, v, 0.0) for m, v in zip(masks, values[kind])]
            rows[kind].append(jnp.sum(parts[0] + parts[1], axis=0, keepdims=True))
    stacked = jnp.concatenate([row for kind in rows for row in kind], axis=0)
    return lax.dot_general(
        jnp.ones((8, 128), F32),
        stacked,
        dimension_numbers=(((1,), (1,)), ((), ())),
        precision=lax.Precision.HIGHEST,
        preferred_element_type=F32,
    )[:1]


def kernel(
    particle_hbm, bin_hbm, slope_hbm, table_hbm, map_ref, power_ref, correlation_ref,
    data, bins, slopes, table, first, middle0, middle1, volume,
    ring_buffer, part, spread_buffer, slab, planes, info_ref, gathered, weight_ref, own, other, swap, stat_plane, stat_line,
    count_ref, first_ref, second_ref,
    local_sem, ring_send, ring_recv, spread_send, spread_recv, plane_send, plane_recv, small_send, small_recv,
):
    half, x, y, z = (lax.axis_index(name) for name in HALF_ROW_COL)
    in_plane, in_line = x * 4 + y, z * 2 + half
    loads = [
        pltpu.make_async_copy(source, target, local_sem.at[index])
        for index, (source, target) in enumerate(
            (
                (bin_hbm, bins),
                (slope_hbm, slopes),
                (table_hbm, table),
                (particle_hbm.at[0], data.at[0]),
                (particle_hbm.at[1], data.at[1]),
            )
        )
    ]
    for load in loads:
        load.start()
    plane_peers, line_peers = others("row_0", "row_1"), others("col", "half")
    barrier = pltpu.get_barrier_semaphore()
    for peer in plane_peers + line_peers:
        pl.semaphore_signal(barrier, inc=1, device_id=peer, device_id_type=MESH)
    loads[0].wait()
    loads[1].wait()
    lane = iota((1, 128), 1)
    info = jnp.zeros((1, 128), jnp.int32)
    for particle in range(2):
        info = jnp.where(lane == particle, bins[particle], info)
        for side in range(2):
            info = jnp.where(lane == 2 + 2 * particle + side, slopes[particle, side], info)
    info_ref[...] = info

    order = owner_rows(x, y)
    loads[2].wait()
    operators = [third_operator(table[bins[particle], 2]) for particle in range(2)]
    second = jnp.concatenate(
        [table[bins[particle], 1].astype(F32) for particle in range(2)], axis=1
    ).astype(BF16)
    for particle in range(2):
        loads[3 + particle].wait()
        along_first(particle, order, bins, slopes, data, table, first)

    rings = [
        [
            Ring4(
                axis,
                lambda group, side, color=color, inner=inner: volume.at[group, color, inner, pl.ds(2 * side, 2)],
                ring_buffer.at[color, inner],
                ring_send.at[color, inner],
                ring_recv.at[color, inner],
            )
            for color, axis in enumerate(("row_0", "row_1"))
        ]
        for inner in range(2)
    ]
    flat = rings[0] + rings[1]
    group = functools.partial(
        insert_group,
        operators=operators, second=second, first=first, middles=(middle0, middle1), volume=volume,
    )
    group(0)
    pl.semaphore_wait(barrier, 30)
    gathered[half, z, in_plane] = info_ref[...]
    info_copies = exchange(
        plane_peers, lambda peer: info_ref, gathered.at[half, z, in_plane], small_send.at[0], small_recv.at[0]
    )
    pending = list(info_copies)
    for ring in flat:
        ring.send_far()
    group(1)
    for ring in flat:
        ring.send_right()
    group(2)
    for ring in flat:
        ring.send_left()
    arrived(info_copies)
    info_copies = exchange(
        line_peers, lambda peer: gathered.at[half, z], gathered.at[half, z], small_send.at[1], small_recv.at[1]
    )
    pending += info_copies
    group(3)
    for ring in rings[0]:
        ring.forward()
    arrived(info_copies)
    bin_counts([gathered[index].reshape(128, 128) for index in range(2)], count_ref)
    for ring in rings[1]:
        ring.forward()
    insert_counts(table, count_ref, first_ref, second_ref)

    own_plane = in_plane * 4 + half * 2
    spreads = []
    for inner in range(2):
        spreads.append([])
        for color, axis in enumerate(("row_1", "row_0")):
            rings[inner][color].finish(part.at[color, inner])
            me = lax.axis_index(axis)
            spreads[inner] += exchange(
                others(axis),
                lambda peer, axis=axis, color=color, inner=inner: part.at[color, inner, peer[axis]],
                spread_buffer.at[color, inner, me],
                spread_send.at[color, inner],
                spread_recv.at[color, inner],
            )
        if inner == 0:
            weight_sums(own_plane, z, table, first_ref, second_ref, weight_ref)
    plane_copies = []
    for inner in range(2):
        arrived(spreads[inner])
        pending += spreads[inner]
        for color, axis in enumerate(("row_1", "row_0")):
            me = lax.axis_index(axis)
            total = part[color, inner, me]
            for step in range(1, 4):
                total = total + spread_buffer[color, inner, (me + step) % 4]
            slab[color, inner] = total
        plane_copies += exchange(
            line_peers,
            lambda peer, inner=inner: slab.at[
                peer["half"], inner, pl.ds(pl.multiple_of(peer["col"] * 8, 8), 8)
            ],
            planes.at[half, inner, z],
            plane_send.at[inner],
            plane_recv.at[inner],
        )
        planes[half, inner, z] = slab[half, inner, pl.ds(pl.multiple_of(z * 8, 8), 8)]
    arrived(plane_copies)
    pending += plane_copies

    maps = [[], []]
    for which in range(2):
        for inner in range(2):
            total = planes[which, inner, 0]
            for index in range(1, 8):
                total = total + planes[which, inner, index]
            maps[which].append(total / (weight_ref[which, inner] + 1.0))
            own[which, inner] = maps[which][inner]
    partner = remote(
        own.at[1 - half], other, small_send.at[4, 0], small_recv.at[4, 0], {"half": 1 - half}
    )
    stat_plane[in_plane] = shell_rows(maps[0], maps[1], own_plane, z)
    copies = exchange(
        plane_peers, lambda peer: stat_plane.at[in_plane], stat_plane.at[in_plane], small_send.at[2], small_recv.at[2]
    )
    pending += copies
    partner.wait_recv()
    for inner in range(2):
        swap[half * 2 + inner] = own[half, inner]
        swap[(1 - half) * 2 + inner] = other[inner]
    low = iota((4, 128), 1) < 64
    for plane in range(4):
        even = swap[plane, pl.ds(0, 4, stride=2), :]
        odd = swap[plane, pl.ds(1, 4, stride=2), :]
        parts = (
            jnp.where(low, even, pltpu.roll(odd, 64, 1)),
            jnp.where(low, pltpu.roll(even, 64, 1), odd),
        )
        for component in range(2):
            for piece in range(4):
                map_ref[0, component, pl.ds(plane, 1), pl.ds(128 * piece, 128)] = parts[component][
                    piece : piece + 1
                ]
    arrived(copies)

    def summed(ref):
        total = ref[0]
        for index in range(1, 16):
            total = total + ref[index]
        return total

    stat_line[in_line] = summed(stat_plane)
    copies = exchange(
        line_peers, lambda peer: stat_line.at[in_line], stat_line.at[in_line], small_send.at[3], small_recv.at[3]
    )
    pending += copies
    arrived(copies)
    stat = jnp.broadcast_to(summed(stat_line), (8, 128))
    power_first, power_second, counts = (pltpu.roll(stat, 128 - 32 * kind, 1) for kind in (1, 2, 3))
    correlation = stat / jnp.sqrt(power_first * power_second + 1e-06)
    power_ref[pl.ds(0, 1), :] = (power_first / counts)[:1, :SHELLS]
    power_ref[pl.ds(1, 1), :] = (power_second / counts)[:1, :SHELLS]
    correlation_ref[...] = correlation[:1, :SHELLS]
    for ring in flat:
        pending += ring.copies
    pending.append(partner)
    for copy in pending:
        copy.wait_send()


def emit_kernel(map_ref, power_ref, correlation_ref, map_out, power_out, correlation_out, sems):
    pairs = ((map_ref, map_out), (power_ref, power_out), (correlation_ref, correlation_out))
    copies = [
        pltpu.make_async_copy(source, target, sems.at[index]) for index, (source, target) in enumerate(pairs)
    ]
    for copy in copies:
        copy.start()
    for copy in copies:
        copy.wait()


def local(particles, orient_bin, tilt_slope, interp_table):
    hbm = pl.BlockSpec(memory_space=pltpu.HBM)
    vmem = pl.BlockSpec(memory_space=pltpu.VMEM)
    dma = pltpu.SemaphoreType.DMA
    f32 = lambda *shape: pltpu.VMEM(shape, F32)
    shapes = (
        jax.ShapeDtypeStruct((1, 2, 4, 512), F32),
        jax.ShapeDtypeStruct((2, SHELLS), F32),
        jax.ShapeDtypeStruct((1, SHELLS), F32),
    )
    results = pl.pallas_call(
        kernel,
        out_shape=tuple(pltpu.VMEM(shape.shape, F32) for shape in shapes),
        in_specs=[hbm] * 4,
        out_specs=(vmem, vmem, vmem),
        scratch_shapes=[
            pltpu.VMEM((2, 2, GRID, GRID * GRID), BF16),
            pltpu.SMEM((2,), jnp.int32),
            pltpu.SMEM((2, 2), jnp.int32),
            pltpu.VMEM((BINS, 3, GRID, GRID), BF16),
            pltpu.VMEM((2, 32, GRID, 256), BF16),
            f32(GRID * STRIDE, 128),
            f32(GRID * STRIDE, 128),
            f32(4, 2, 2, 4, GRID, 128),
            f32(2, 2, 6, 2, GRID, 128),
            f32(2, 2, 4, GRID, 128),
            f32(2, 2, 4, GRID, 128),
            f32(2, 2, GRID, 128),
            f32(2, 2, 8, 8, 128),
            pltpu.VMEM((1, 128), jnp.int32),
            pltpu.VMEM((2, 8, 16, 1, 128), jnp.int32),
            f32(2, 2, 8, 128),
            f32(2, 2, 8, 128),
            f32(2, 8, 128),
            f32(4, 8, 128),
            f32(16, 1, 128),
            f32(16, 1, 128),
            f32((GRID + 1) * 2 * BINS, 128),
            f32(2, BINS, GRID, 128),
            f32(GRID, 128),
            dma((5,)),
            dma((2, 2, 6)),
            dma((2, 2, 6)),
            dma((2, 2, 4)),
            dma((2, 2, 4)),
            dma((2, 16)),
            dma((2, 16)),
            dma((5, 16)),
            dma((5, 16)),
        ],
        compiler_params=pltpu.CompilerParams(
            collective_id=0, has_side_effects=True, vmem_limit_bytes=60 * 2**20
        ),
        name="halfmaps",
    )(particles, orient_bin, tilt_slope, interp_table)
    return pl.pallas_call(
        emit_kernel,
        out_shape=shapes,
        in_specs=[vmem] * 3,
        out_specs=(hbm,) * 3,
        scratch_shapes=[dma((3,))],
        compiler_params=pltpu.CompilerParams(vmem_limit_bytes=2**20),
        name="emit",
    )(*results)


def solution(mesh):
    torus = Mesh(
        mesh.devices.reshape(mesh.shape["half"], 4, 4, mesh.shape["col"]), HALF_ROW_COL
    )
    in_specs = (P(HALF_ROW_COL, None, None, None), P(HALF_ROW_COL), P(HALF_ROW_COL, None), P())
    out_specs = (P("half", None, ("row_0", "row_1"), "col"), P(), P("half", None))
    return jax.shard_map(local, mesh=torus, in_specs=in_specs, out_specs=out_specs, check_vma=False)
```

```python
import functools
import itertools

import jax
import jax.numpy as jnp
from jax import lax
from jax.experimental import pallas as pl
from jax.experimental.pallas import tpu as pltpu
from jax.sharding import Mesh
from jax.sharding import PartitionSpec as P

SHELLS = 29
GRID = 64
BINS = 16
STRIDE = 24
SIZES = {"half": 2, "row_0": 4, "row_1": 4, "col": 8}
HALF_ROW_COL = ("half", "row_0", "row_1", "col")
MESH = pl.DeviceIdType.MESH
F32 = jnp.float32
BF16 = jnp.bfloat16


def iota(shape, dim):
    return lax.broadcasted_iota(jnp.int32, shape, dim)


def owner_rows(x, y):
    index = iota((GRID, GRID), 0)
    group, color, other, inner = index // 16, (index // 8) % 2, (index // 2) % 4, index % 2
    shift = jnp.where(group == 0, 2, jnp.where(group == 1, 1, jnp.where(group == 2, 3, 0)))
    main = (jnp.where(color == 0, x, y) + shift) % 4
    plane = jnp.where(color == 0, 16 * main + 4 * other, 16 * other + 4 * main + 2) + inner
    return (plane == iota((GRID, GRID), 1)).astype(F32).astype(BF16)


def along_first(particle, order, bins, slopes, data, table, first):
    wave_first = iota((GRID, 128), 0) - 32
    wave_third = (iota((GRID, 128), 1) & 63) - 32
    limit = jnp.where(wave_first * wave_third >= 0, slopes[particle, 0], slopes[particle, 1])
    inside = 16 * jnp.abs(wave_third) <= limit * jnp.abs(wave_first)
    weight = inside.astype(F32).astype(BF16)
    kernel = jnp.dot(order, table[bins[particle], 0], preferred_element_type=F32).astype(BF16)

    def pairs(step, carry):
        for inner in range(16):
            pair = step * 16 + inner
            columns = pl.ds(pl.multiple_of(pair * 128, 128), 128)
            both = jnp.concatenate([data[particle, part, :, columns] * weight for part in range(2)], axis=1)
            first[particle, pair] = jnp.dot(kernel, both, preferred_element_type=F32).astype(BF16)
        return carry

    lax.fori_loop(0, 2, pairs, 0)


def third_operator(kernel):
    block_row = iota((256, 256), 0) // 64
    block_col = iota((256, 256), 1) // 64
    matching = (block_row // 2 == block_col % 2) & (block_row % 2 == block_col // 2)
    third = jnp.transpose(kernel.astype(F32))
    third = jnp.concatenate([third, third], axis=1)
    third = jnp.concatenate([third, third], axis=1)
    third = jnp.concatenate([third, third, third, third], axis=0)
    return jnp.where(matching, third, 0.0).astype(BF16)


def insert_group(group, operators, second, first, middles, volume):
    rows = pl.ds(16 * group, 16)
    for particle, middle in enumerate(middles):
        lines = first[particle, :, rows, :].reshape(512, 256)
        lines = jnp.dot(lines, operators[particle], preferred_element_type=F32)
        for pair in range(32):
            middle[pl.ds(2 * pair * STRIDE, 16), :] = lines[16 * pair : 16 * pair + 16, :128]
            middle[pl.ds((2 * pair + 1) * STRIDE, 16), :] = lines[16 * pair : 16 * pair + 16, 128:]
    for place in range(8):
        planes = []
        for inner in range(2):
            sides = [middle[pl.ds(2 * place + inner, GRID, stride=STRIDE), :] for middle in middles]
            planes.append(jnp.concatenate(sides, axis=0).astype(BF16))
        slab = jnp.dot(second, jnp.concatenate(planes, axis=1), preferred_element_type=F32)
        for inner in range(2):
            volume[group, place // 4, inner, place % 4] = slab[:, 128 * inner : 128 * inner + 128]


def bin_counts(infos, count_ref):
    contract = functools.partial(
        lax.dot_general, dimension_numbers=(((1,), (1,)), ((), ())), preferred_element_type=F32
    )
    bin_index = iota((BINS, 128), 0).astype(F32)
    slope_index = iota((GRID, 128), 0).astype(F32)
    parts = [[], []]
    for info in infos:
        fields = jnp.transpose(info.astype(F32))[:8]
        bins = [(fields[particle : particle + 1] == bin_index).astype(F32) for particle in range(2)]
        bins = jnp.concatenate(bins, axis=1).astype(BF16)
        for side in range(2):
            slopes = [
                (fields[2 + 2 * particle + side : 3 + 2 * particle + side] == slope_index).astype(F32)
                for particle in range(2)
            ]
            parts[side].append(contract(bins, jnp.concatenate(slopes, axis=1).astype(BF16)))
    histogram = jnp.concatenate(parts[0] + parts[1], axis=0).astype(BF16)

    reach = (16 * jnp.abs((iota((GRID, 128), 1) & 63) - 32)).astype(F32)
    wave_third = (iota((2 * BINS, 128), 1) & 63) - 32
    nonneg, nonpos = wave_third >= 0, wave_third <= 0

    def counted(distance):
        inside = (reach <= slope_index * distance).astype(F32).astype(BF16)
        counts = jnp.dot(histogram, inside, preferred_element_type=F32)
        return counts[: 2 * BINS], counts[2 * BINS :]

    def place(first):
        return pl.ds(pl.multiple_of(first * 2 * BINS, 2 * BINS), 2 * BINS)

    def planes(step, carry):
        for inner in range(8):
            distance = step * 8 + inner + 1
            same, opposite = counted(distance.astype(F32))
            count_ref[place(32 + distance), :] = jnp.where(nonneg, same, opposite)
            count_ref[place(32 - distance), :] = jnp.where(nonpos, same, opposite)
        return carry

    count_ref[place(32), :] = counted(0.0)[0]
    lax.fori_loop(0, 4, planes, 0)


def insert_counts(table, count_ref, first_ref, second_ref):
    bin_lane = iota((GRID, 128), 1)
    second = jnp.zeros((GRID, 128), F32)
    for which in range(BINS):
        counts = [count_ref[pl.ds(BINS * half + which, GRID, stride=2 * BINS), :] for half in range(2)]
        counts = jnp.concatenate(counts, axis=1).astype(BF16)
        lines = jnp.dot(table[which, 0], counts, preferred_element_type=F32)
        for half in range(2):
            first_ref[half, which] = lines[:, 128 * half : 128 * half + 128]
        total = jnp.sum(table[which, 1].astype(F32), axis=1, keepdims=True)
        second = jnp.where(bin_lane == which, total, second)
    second_ref[...] = second


def weight_sums(plane, col, table, first_ref, second_ref, weight_ref):
    second = second_ref[pl.ds(pl.multiple_of(col * 8, 8), 8), :]
    contract = functools.partial(
        lax.dot_general, dimension_numbers=(((1,), (1,)), ((), ())), preferred_element_type=F32
    )
    sums = [jnp.zeros((8, 128), F32) for _ in range(4)]
    for which in range(BINS):
        first = jnp.concatenate([first_ref[half, which, pl.ds(plane, 2), :] for half in range(2)], axis=0)[:, :GRID]
        high = first.astype(BF16)
        low = (first - high.astype(F32)).astype(BF16)
        third = jnp.concatenate([table[which, 2]] * 2, axis=0)
        lines = contract(high, third) + contract(low, third)
        for index in range(4):
            sums[index] = sums[index] + second[:, which : which + 1] * lines[index : index + 1]
    for index in range(4):
        weight_ref[index // 2, index % 2] = sums[index]


def remote(source, target, send, recv, device):
    copy = pltpu.make_async_remote_copy(
        src_ref=source, dst_ref=target, send_sem=send, recv_sem=recv, device_id=device, device_id_type=MESH
    )
    copy.start()
    return copy


class Ring4:
    def __init__(self, axis, source, buffer, send, recv):
        self.axis, self.source, self.buffer, self.send, self.recv = axis, source, buffer, send, recv
        me = lax.axis_index(axis)
        self.right, self.left = (me + 1) % 4, (me + 3) % 4
        self.copies = [None] * 6

    def copy(self, slot, source, target):
        self.copies[slot] = remote(
            source, self.buffer.at[slot], self.send.at[slot], self.recv.at[slot], {self.axis: target}
        )

    def send_far(self):
        self.copy(0, self.source(0, 0), self.right)
        self.copy(3, self.source(0, 1), self.left)

    def send_right(self):
        self.copy(2, self.source(1, 1), self.right)

    def send_left(self):
        self.copy(5, self.source(2, 0), self.left)

    def forward(self):
        self.copies[0].wait_recv()
        self.buffer[0] = self.buffer[0] + self.source(1, 0)[...]
        self.copy(1, self.buffer.at[0], self.right)
        self.copies[3].wait_recv()
        self.buffer[3] = self.buffer[3] + self.source(2, 1)[...]
        self.copy(4, self.buffer.at[3], self.left)

    def finish(self, result):
        for half, near, other in ((0, 1, 5), (1, 4, 2)):
            self.copies[other].wait_recv()
            self.copies[near].wait_recv()
            result[pl.ds(2 * half, 2)] = (
                self.source(3, half)[...] + self.buffer[near] + self.buffer[other]
            )


def hops(offset, sizes):
    return sum(min(step, size - step) for step, size in zip(offset, sizes))


def others(*axes):
    sizes = [SIZES[axis] for axis in axes]
    offsets = [offset for offset in itertools.product(*map(range, sizes)) if any(offset)]
    offsets.sort(key=lambda offset: -hops(offset, sizes))
    places = {
        axis: [lax.rem(lax.axis_index(axis) + step, size) for step in range(size)]
        for axis, size in zip(axes, sizes)
    }
    return [{axis: places[axis][step] for axis, step in zip(axes, offset)} for offset in offsets]


def exchange(peers, source, target, send, recv):
    return [
        remote(source(peer), target, send.at[index], recv.at[index], peer) for index, peer in enumerate(peers)
    ]


def arrived(copies):
    for copy in copies:
        copy.wait_recv()


def shell_rows(sums_first, sums_second, plane, col):
    wave_second = iota((8, 128), 0) + col * 8 - 32
    wave_third = (iota((8, 128), 1) & 63) - 32
    rest = wave_second * wave_second + wave_third * wave_third
    radius = []
    for index in range(2):
        wave_first = plane + index - 32
        radius.append(rest + wave_first * wave_first)
    real = iota((8, 128), 1) < 64
    values = [
        [first * second for first, second in zip(sums_first, sums_second)],
        [first * first for first in sums_first],
        [second * second for second in sums_second],
        [jnp.where(real, 1.0, 0.0).astype(F32)] * 2,
    ]
    rows = [[] for _ in range(4)]
    for shell in range(32):
        low = 0 if shell == 0 else (shell + 3) ** 2
        high = (shell + 4) ** 2 if shell < SHELLS else low
        masks = [(r >= low) & (r < high) for r in radius]
        for kind in range(4):
            parts = [jnp.where(m, v, 0.0) for m, v in zip(masks, values[kind])]
            rows[kind].append(jnp.sum(parts[0] + parts[1], axis=0, keepdims=True))
    stacked = jnp.concatenate([row for kind in rows for row in kind], axis=0)
    return lax.dot_general(
        jnp.ones((8, 128), F32),
        stacked,
        dimension_numbers=(((1,), (1,)), ((), ())),
        precision=lax.Precision.HIGHEST,
        preferred_element_type=F32,
    )[:1]


def kernel(
    particle_hbm, bin_hbm, slope_hbm, table_hbm, map_ref, power_ref, correlation_ref,
    data, bins, slopes, table, first, middle0, middle1, volume,
    ring_buffer, part, spread_buffer, slab, planes, info_ref, gathered, weight_ref, own, other, swap, stat_plane, stat_line,
    count_ref, first_ref, second_ref,
    local_sem, ring_send, ring_recv, spread_send, spread_recv, plane_send, plane_recv, small_send, small_recv,
):
    half, x, y, z = (lax.axis_index(name) for name in HALF_ROW_COL)
    in_plane, in_line = x * 4 + y, z * 2 + half
    loads = [
        pltpu.make_async_copy(source, target, local_sem.at[index])
        for index, (source, target) in enumerate(
            (
                (bin_hbm, bins),
                (slope_hbm, slopes),
                (table_hbm, table),
                (particle_hbm.at[0], data.at[0]),
                (particle_hbm.at[1], data.at[1]),
            )
        )
    ]
    for load in loads:
        load.start()
    plane_peers, line_peers = others("row_0", "row_1"), others("col", "half")
    barrier = pltpu.get_barrier_semaphore()
    for peer in plane_peers + line_peers:
        pl.semaphore_signal(barrier, inc=1, device_id=peer, device_id_type=MESH)
    loads[0].wait()
    loads[1].wait()
    lane = iota((1, 128), 1)
    info = jnp.zeros((1, 128), jnp.int32)
    for particle in range(2):
        info = jnp.where(lane == particle, bins[particle], info)
        for side in range(2):
            info = jnp.where(lane == 2 + 2 * particle + side, slopes[particle, side], info)
    info_ref[...] = info

    order = owner_rows(x, y)
    loads[2].wait()
    operators = [third_operator(table[bins[particle], 2]) for particle in range(2)]
    second = jnp.concatenate(
        [table[bins[particle], 1].astype(F32) for particle in range(2)], axis=1
    ).astype(BF16)
    for particle in range(2):
        loads[3 + particle].wait()
        along_first(particle, order, bins, slopes, data, table, first)

    rings = [
        [
            Ring4(
                axis,
                lambda group, side, color=color, inner=inner: volume.at[group, color, inner, pl.ds(2 * side, 2)],
                ring_buffer.at[color, inner],
                ring_send.at[color, inner],
                ring_recv.at[color, inner],
            )
            for color, axis in enumerate(("row_0", "row_1"))
        ]
        for inner in range(2)
    ]
    flat = rings[0] + rings[1]
    group = functools.partial(
        insert_group,
        operators=operators, second=second, first=first, middles=(middle0, middle1), volume=volume,
    )
    group(0)
    pl.semaphore_wait(barrier, 30)
    gathered[half, z, in_plane] = info_ref[...]
    info_copies = exchange(
        plane_peers, lambda peer: info_ref, gathered.at[half, z, in_plane], small_send.at[0], small_recv.at[0]
    )
    pending = list(info_copies)
    for ring in flat:
        ring.send_far()
    group(1)
    for ring in flat:
        ring.send_right()
    group(2)
    for ring in flat:
        ring.send_left()
    group(3)
    for ring in flat:
        ring.forward()
    arrived(info_copies)
    info_copies = exchange(
        line_peers, lambda peer: gathered.at[half, z], gathered.at[half, z], small_send.at[1], small_recv.at[1]
    )
    pending += info_copies

    own_plane = in_plane * 4 + half * 2
    spreads = []
    for inner in range(2):
        spreads.append([])
        for color, axis in enumerate(("row_1", "row_0")):
            rings[inner][color].finish(part.at[color, inner])
            me = lax.axis_index(axis)
            spreads[inner] += exchange(
                others(axis),
                lambda peer, axis=axis, color=color, inner=inner: part.at[color, inner, peer[axis]],
                spread_buffer.at[color, inner, me],
                spread_send.at[color, inner],
                spread_recv.at[color, inner],
            )
    plane_copies = []
    for inner in range(2):
        arrived(spreads[inner])
        pending += spreads[inner]
        for color, axis in enumerate(("row_1", "row_0")):
            me = lax.axis_index(axis)
            total = part[color, inner, me]
            for step in range(1, 4):
                total = total + spread_buffer[color, inner, (me + step) % 4]
            slab[color, inner] = total
        plane_copies += exchange(
            line_peers,
            lambda peer, inner=inner: slab.at[
                peer["half"], inner, pl.ds(pl.multiple_of(peer["col"] * 8, 8), 8)
            ],
            planes.at[half, inner, z],
            plane_send.at[inner],
            plane_recv.at[inner],
        )
        planes[half, inner, z] = slab[half, inner, pl.ds(pl.multiple_of(z * 8, 8), 8)]
        if inner == 0:
            arrived(info_copies)
            bin_counts([gathered[index].reshape(128, 128) for index in range(2)], count_ref)
            insert_counts(table, count_ref, first_ref, second_ref)
        else:
            weight_sums(own_plane, z, table, first_ref, second_ref, weight_ref)
    arrived(plane_copies)
    pending += plane_copies

    maps = [[], []]
    for which in range(2):
        for inner in range(2):
            total = planes[which, inner, 0]
            for index in range(1, 8):
                total = total + planes[which, inner, index]
            maps[which].append(total / (weight_ref[which, inner] + 1.0))
            own[which, inner] = maps[which][inner]
    partner = remote(
        own.at[1 - half], other, small_send.at[4, 0], small_recv.at[4, 0], {"half": 1 - half}
    )
    stat_plane[in_plane] = shell_rows(maps[0], maps[1], own_plane, z)
    copies = exchange(
        plane_peers, lambda peer: stat_plane.at[in_plane], stat_plane.at[in_plane], small_send.at[2], small_recv.at[2]
    )
    pending += copies
    partner.wait_recv()
    for inner in range(2):
        swap[half * 2 + inner] = own[half, inner]
        swap[(1 - half) * 2 + inner] = other[inner]
    low = iota((4, 128), 1) < 64
    for plane in range(4):
        even = swap[plane, pl.ds(0, 4, stride=2), :]
        odd = swap[plane, pl.ds(1, 4, stride=2), :]
        parts = (
            jnp.where(low, even, pltpu.roll(odd, 64, 1)),
            jnp.where(low, pltpu.roll(even, 64, 1), odd),
        )
        for component in range(2):
            for piece in range(4):
                map_ref[0, component, pl.ds(plane, 1), pl.ds(128 * piece, 128)] = parts[component][
                    piece : piece + 1
                ]
    arrived(copies)

    def summed(ref):
        total = ref[0]
        for index in range(1, 16):
            total = total + ref[index]
        return total

    stat_line[in_line] = summed(stat_plane)
    copies = exchange(
        line_peers, lambda peer: stat_line.at[in_line], stat_line.at[in_line], small_send.at[3], small_recv.at[3]
    )
    pending += copies
    arrived(copies)
    stat = jnp.broadcast_to(summed(stat_line), (8, 128))
    power_first, power_second, counts = (pltpu.roll(stat, 128 - 32 * kind, 1) for kind in (1, 2, 3))
    correlation = stat / jnp.sqrt(power_first * power_second + 1e-06)
    power_ref[pl.ds(0, 1), :] = (power_first / counts)[:1, :SHELLS]
    power_ref[pl.ds(1, 1), :] = (power_second / counts)[:1, :SHELLS]
    correlation_ref[...] = correlation[:1, :SHELLS]
    for ring in flat:
        pending += ring.copies
    pending.append(partner)
    for copy in pending:
        copy.wait_send()


def emit_kernel(map_ref, power_ref, correlation_ref, map_out, power_out, correlation_out, sems):
    pairs = ((map_ref, map_out), (power_ref, power_out), (correlation_ref, correlation_out))
    copies = [
        pltpu.make_async_copy(source, target, sems.at[index]) for index, (source, target) in enumerate(pairs)
    ]
    for copy in copies:
        copy.start()
    for copy in copies:
        copy.wait()


def local(particles, orient_bin, tilt_slope, interp_table):
    hbm = pl.BlockSpec(memory_space=pltpu.HBM)
    vmem = pl.BlockSpec(memory_space=pltpu.VMEM)
    dma = pltpu.SemaphoreType.DMA
    f32 = lambda *shape: pltpu.VMEM(shape, F32)
    shapes = (
        jax.ShapeDtypeStruct((1, 2, 4, 512), F32),
        jax.ShapeDtypeStruct((2, SHELLS), F32),
        jax.ShapeDtypeStruct((1, SHELLS), F32),
    )
    results = pl.pallas_call(
        kernel,
        out_shape=tuple(pltpu.VMEM(shape.shape, F32) for shape in shapes),
        in_specs=[hbm] * 4,
        out_specs=(vmem, vmem, vmem),
        scratch_shapes=[
            pltpu.VMEM((2, 2, GRID, GRID * GRID), BF16),
            pltpu.SMEM((2,), jnp.int32),
            pltpu.SMEM((2, 2), jnp.int32),
            pltpu.VMEM((BINS, 3, GRID, GRID), BF16),
            pltpu.VMEM((2, 32, GRID, 256), BF16),
            f32(GRID * STRIDE, 128),
            f32(GRID * STRIDE, 128),
            f32(4, 2, 2, 4, GRID, 128),
            f32(2, 2, 6, 2, GRID, 128),
            f32(2, 2, 4, GRID, 128),
            f32(2, 2, 4, GRID, 128),
            f32(2, 2, GRID, 128),
            f32(2, 2, 8, 8, 128),
            pltpu.VMEM((1, 128), jnp.int32),
            pltpu.VMEM((2, 8, 16, 1, 128), jnp.int32),
            f32(2, 2, 8, 128),
            f32(2, 2, 8, 128),
            f32(2, 8, 128),
            f32(4, 8, 128),
            f32(16, 1, 128),
            f32(16, 1, 128),
            f32((GRID + 1) * 2 * BINS, 128),
            f32(2, BINS, GRID, 128),
            f32(GRID, 128),
            dma((5,)),
            dma((2, 2, 6)),
            dma((2, 2, 6)),
            dma((2, 2, 4)),
            dma((2, 2, 4)),
            dma((2, 16)),
            dma((2, 16)),
            dma((5, 16)),
            dma((5, 16)),
        ],
        compiler_params=pltpu.CompilerParams(
            collective_id=0, has_side_effects=True, vmem_limit_bytes=60 * 2**20
        ),
        name="halfmaps",
    )(particles, orient_bin, tilt_slope, interp_table)
    return pl.pallas_call(
        emit_kernel,
        out_shape=shapes,
        in_specs=[vmem] * 3,
        out_specs=(hbm,) * 3,
        scratch_shapes=[dma((3,))],
        compiler_params=pltpu.CompilerParams(vmem_limit_bytes=2**20),
        name="emit",
    )(*results)


def solution(mesh):
    torus = Mesh(
        mesh.devices.reshape(mesh.shape["half"], 4, 4, mesh.shape["col"]), HALF_ROW_COL
    )
    in_specs = (P(HALF_ROW_COL, None, None, None), P(HALF_ROW_COL), P(HALF_ROW_COL, None), P())
    out_specs = (P("half", None, ("row_0", "row_1"), "col"), P(), P("half", None))
    return jax.shard_map(local, mesh=torus, in_specs=in_specs, out_specs=out_specs, check_vma=False)
```

```python
import functools
import itertools

import jax
import jax.numpy as jnp
from jax import lax
from jax.experimental import pallas as pl
from jax.experimental.pallas import tpu as pltpu
from jax.sharding import Mesh
from jax.sharding import PartitionSpec as P

SHELLS = 29
GRID = 64
BINS = 16
STRIDE = 24
SIZES = {"half": 2, "row_0": 4, "row_1": 4, "col": 8}
HALF_ROW_COL = ("half", "row_0", "row_1", "col")
MESH = pl.DeviceIdType.MESH
F32 = jnp.float32
BF16 = jnp.bfloat16


def iota(shape, dim):
    return lax.broadcasted_iota(jnp.int32, shape, dim)


def owner_rows(x, y):
    index = iota((GRID, GRID), 0)
    group, color, other, inner = index // 16, (index // 8) % 2, (index // 2) % 4, index % 2
    shift = jnp.where(group == 0, 2, jnp.where(group == 1, 1, jnp.where(group == 2, 3, 0)))
    main = (jnp.where(color == 0, x, y) + shift) % 4
    plane = jnp.where(color == 0, 16 * main + 4 * other, 16 * other + 4 * main + 2) + inner
    return (plane == iota((GRID, GRID), 1)).astype(F32).astype(BF16)


def along_first(particle, order, bins, slopes, data, table, first):
    wave_first = iota((GRID, 128), 0) - 32
    wave_third = (iota((GRID, 128), 1) & 63) - 32
    limit = jnp.where(wave_first * wave_third >= 0, slopes[particle, 0], slopes[particle, 1])
    inside = 16 * jnp.abs(wave_third) <= limit * jnp.abs(wave_first)
    weight = inside.astype(F32).astype(BF16)
    kernel = jnp.dot(order, table[bins[particle], 0], preferred_element_type=F32).astype(BF16)

    def pairs(step, carry):
        for inner in range(16):
            pair = step * 16 + inner
            columns = pl.ds(pl.multiple_of(pair * 128, 128), 128)
            both = jnp.concatenate([data[particle, part, :, columns] * weight for part in range(2)], axis=1)
            first[particle, pair] = jnp.dot(kernel, both, preferred_element_type=F32).astype(BF16)
        return carry

    lax.fori_loop(0, 2, pairs, 0)


def third_operator(kernel):
    block_row = iota((256, 256), 0) // 64
    block_col = iota((256, 256), 1) // 64
    matching = (block_row // 2 == block_col % 2) & (block_row % 2 == block_col // 2)
    third = jnp.transpose(kernel.astype(F32))
    third = jnp.concatenate([third, third], axis=1)
    third = jnp.concatenate([third, third], axis=1)
    third = jnp.concatenate([third, third, third, third], axis=0)
    return jnp.where(matching, third, 0.0).astype(BF16)


def insert_group(group, operators, second, first, middles, volume):
    rows = pl.ds(16 * group, 16)
    for particle, middle in enumerate(middles):
        lines = first[particle, :, rows, :].reshape(512, 256)
        lines = jnp.dot(lines, operators[particle], preferred_element_type=F32)
        for pair in range(32):
            middle[pl.ds(2 * pair * STRIDE, 16), :] = lines[16 * pair : 16 * pair + 16, :128]
            middle[pl.ds((2 * pair + 1) * STRIDE, 16), :] = lines[16 * pair : 16 * pair + 16, 128:]
    for place in range(8):
        planes = []
        for inner in range(2):
            sides = [middle[pl.ds(2 * place + inner, GRID, stride=STRIDE), :] for middle in middles]
            planes.append(jnp.concatenate(sides, axis=0).astype(BF16))
        slab = jnp.dot(second, jnp.concatenate(planes, axis=1), preferred_element_type=F32)
        for inner in range(2):
            volume[group, place // 4, inner, place % 4] = slab[:, 128 * inner : 128 * inner + 128]


def bin_counts(infos, count_ref):
    contract = functools.partial(
        lax.dot_general, dimension_numbers=(((1,), (1,)), ((), ())), preferred_element_type=F32
    )
    bin_index = iota((BINS, 128), 0).astype(F32)
    slope_index = iota((GRID, 128), 0).astype(F32)
    parts = [[], []]
    for info in infos:
        fields = jnp.transpose(info.astype(F32))[:8]
        bins = [(fields[particle : particle + 1] == bin_index).astype(F32) for particle in range(2)]
        bins = jnp.concatenate(bins, axis=1).astype(BF16)
        for side in range(2):
            slopes = [
                (fields[2 + 2 * particle + side : 3 + 2 * particle + side] == slope_index).astype(F32)
                for particle in range(2)
            ]
            parts[side].append(contract(bins, jnp.concatenate(slopes, axis=1).astype(BF16)))
    histogram = jnp.concatenate(parts[0] + parts[1], axis=0).astype(BF16)

    reach = (16 * jnp.abs((iota((GRID, 128), 1) & 63) - 32)).astype(F32)
    wave_third = (iota((2 * BINS, 128), 1) & 63) - 32
    nonneg, nonpos = wave_third >= 0, wave_third <= 0

    def counted(distance):
        inside = (reach <= slope_index * distance).astype(F32).astype(BF16)
        counts = jnp.dot(histogram, inside, preferred_element_type=F32)
        return counts[: 2 * BINS], counts[2 * BINS :]

    def place(first):
        return pl.ds(pl.multiple_of(first * 2 * BINS, 2 * BINS), 2 * BINS)

    def planes(step, carry):
        for inner in range(8):
            distance = step * 8 + inner + 1
            same, opposite = counted(distance.astype(F32))
            count_ref[place(32 + distance), :] = jnp.where(nonneg, same, opposite)
            count_ref[place(32 - distance), :] = jnp.where(nonpos, same, opposite)
        return carry

    count_ref[place(32), :] = counted(0.0)[0]
    lax.fori_loop(0, 4, planes, 0)


def insert_counts(table, count_ref, first_ref, second_ref):
    bin_lane = iota((GRID, 128), 1)
    second = jnp.zeros((GRID, 128), F32)
    for which in range(BINS):
        counts = [count_ref[pl.ds(BINS * half + which, GRID, stride=2 * BINS), :] for half in range(2)]
        counts = jnp.concatenate(counts, axis=1).astype(BF16)
        lines = jnp.dot(table[which, 0], counts, preferred_element_type=F32)
        for half in range(2):
            first_ref[half, which] = lines[:, 128 * half : 128 * half + 128]
        total = jnp.sum(table[which, 1].astype(F32), axis=1, keepdims=True)
        second = jnp.where(bin_lane == which, total, second)
    second_ref[...] = second


def weight_sums(plane, col, table, first_ref, second_ref, weight_ref):
    second = second_ref[pl.ds(pl.multiple_of(col * 8, 8), 8), :]
    contract = functools.partial(
        lax.dot_general, dimension_numbers=(((1,), (1,)), ((), ())), preferred_element_type=F32
    )
    sums = [jnp.zeros((8, 128), F32) for _ in range(4)]
    for which in range(BINS):
        first = jnp.concatenate([first_ref[half, which, pl.ds(plane, 2), :] for half in range(2)], axis=0)[:, :GRID]
        high = first.astype(BF16)
        low = (first - high.astype(F32)).astype(BF16)
        third = jnp.concatenate([table[which, 2]] * 2, axis=0)
        lines = contract(high, third) + contract(low, third)
        for index in range(4):
            sums[index] = sums[index] + second[:, which : which + 1] * lines[index : index + 1]
    for index in range(4):
        weight_ref[index // 2, index % 2] = sums[index]


def remote(source, target, send, recv, device):
    copy = pltpu.make_async_remote_copy(
        src_ref=source, dst_ref=target, send_sem=send, recv_sem=recv, device_id=device, device_id_type=MESH
    )
    copy.start()
    return copy


class Ring4:
    def __init__(self, axis, source, buffer, send, recv):
        self.axis, self.source, self.buffer, self.send, self.recv = axis, source, buffer, send, recv
        me = lax.axis_index(axis)
        self.right, self.left = (me + 1) % 4, (me + 3) % 4
        self.copies = [None] * 6

    def copy(self, slot, source, target):
        self.copies[slot] = remote(
            source, self.buffer.at[slot], self.send.at[slot], self.recv.at[slot], {self.axis: target}
        )

    def send_far(self):
        self.copy(0, self.source(0, 0), self.right)
        self.copy(3, self.source(0, 1), self.left)

    def send_right(self):
        self.copy(2, self.source(1, 1), self.right)

    def send_left(self):
        self.copy(5, self.source(2, 0), self.left)

    def forward(self):
        self.copies[0].wait_recv()
        self.buffer[0] = self.buffer[0] + self.source(1, 0)[...]
        self.copy(1, self.buffer.at[0], self.right)
        self.copies[3].wait_recv()
        self.buffer[3] = self.buffer[3] + self.source(2, 1)[...]
        self.copy(4, self.buffer.at[3], self.left)

    def finish(self, result):
        for half, near, other in ((0, 1, 5), (1, 4, 2)):
            self.copies[other].wait_recv()
            self.copies[near].wait_recv()
            result[pl.ds(2 * half, 2)] = (
                self.source(3, half)[...] + self.buffer[near] + self.buffer[other]
            )


def hops(offset, sizes):
    return sum(min(step, size - step) for step, size in zip(offset, sizes))


def others(*axes):
    sizes = [SIZES[axis] for axis in axes]
    offsets = [offset for offset in itertools.product(*map(range, sizes)) if any(offset)]
    offsets.sort(key=lambda offset: -hops(offset, sizes))
    places = {
        axis: [lax.rem(lax.axis_index(axis) + step, size) for step in range(size)]
        for axis, size in zip(axes, sizes)
    }
    return [{axis: places[axis][step] for axis, step in zip(axes, offset)} for offset in offsets]


def exchange(peers, source, target, send, recv):
    return [
        remote(source(peer), target, send.at[index], recv.at[index], peer) for index, peer in enumerate(peers)
    ]


def arrived(copies):
    for copy in copies:
        copy.wait_recv()


def shell_rows(sums_first, sums_second, plane, col):
    wave_second = iota((8, 128), 0) + col * 8 - 32
    wave_third = (iota((8, 128), 1) & 63) - 32
    rest = wave_second * wave_second + wave_third * wave_third
    radius = []
    for index in range(2):
        wave_first = plane + index - 32
        radius.append(rest + wave_first * wave_first)
    real = iota((8, 128), 1) < 64
    values = [
        [first * second for first, second in zip(sums_first, sums_second)],
        [first * first for first in sums_first],
        [second * second for second in sums_second],
        [jnp.where(real, 1.0, 0.0).astype(F32)] * 2,
    ]
    rows = [[] for _ in range(4)]
    for shell in range(32):
        low = 0 if shell == 0 else (shell + 3) ** 2
        high = (shell + 4) ** 2 if shell < SHELLS else low
        masks = [(r >= low) & (r < high) for r in radius]
        for kind in range(4):
            parts = [jnp.where(m, v, 0.0) for m, v in zip(masks, values[kind])]
            rows[kind].append(jnp.sum(parts[0] + parts[1], axis=0, keepdims=True))
    stacked = jnp.concatenate([row for kind in rows for row in kind], axis=0)
    return lax.dot_general(
        jnp.ones((8, 128), F32),
        stacked,
        dimension_numbers=(((1,), (1,)), ((), ())),
        precision=lax.Precision.HIGHEST,
        preferred_element_type=F32,
    )[:1]


def kernel(
    particle_hbm, bin_hbm, slope_hbm, table_hbm, map_ref, power_ref, correlation_ref,
    data, bins, slopes, table, first, middle0, middle1, volume,
    ring_buffer, part, spread_buffer, slab, planes, info_ref, gathered, weight_ref, own, other, swap, stat_all,
    count_ref, first_ref, second_ref,
    local_sem, ring_send, ring_recv, spread_send, spread_recv, plane_send, plane_recv, small_send, small_recv, stat_sem,
):
    half, x, y, z = (lax.axis_index(name) for name in HALF_ROW_COL)
    in_plane, in_line = x * 4 + y, z * 2 + half
    loads = [
        pltpu.make_async_copy(source, target, local_sem.at[index])
        for index, (source, target) in enumerate(
            (
                (bin_hbm, bins),
                (slope_hbm, slopes),
                (table_hbm, table),
                (particle_hbm.at[0], data.at[0]),
                (particle_hbm.at[1], data.at[1]),
            )
        )
    ]
    for load in loads:
        load.start()
    plane_peers, line_peers = others("row_0", "row_1"), others("col", "half")
    barrier = pltpu.get_barrier_semaphore()
    for peer in plane_peers + line_peers:
        pl.semaphore_signal(barrier, inc=1, device_id=peer, device_id_type=MESH)
    loads[0].wait()
    loads[1].wait()
    lane = iota((1, 128), 1)
    info = jnp.zeros((1, 128), jnp.int32)
    for particle in range(2):
        info = jnp.where(lane == particle, bins[particle], info)
        for side in range(2):
            info = jnp.where(lane == 2 + 2 * particle + side, slopes[particle, side], info)
    info_ref[...] = info

    order = owner_rows(x, y)
    loads[2].wait()
    operators = [third_operator(table[bins[particle], 2]) for particle in range(2)]
    second = jnp.concatenate(
        [table[bins[particle], 1].astype(F32) for particle in range(2)], axis=1
    ).astype(BF16)
    for particle in range(2):
        loads[3 + particle].wait()
        along_first(particle, order, bins, slopes, data, table, first)

    rings = [
        [
            Ring4(
                axis,
                lambda group, side, color=color, inner=inner: volume.at[group, color, inner, pl.ds(2 * side, 2)],
                ring_buffer.at[color, inner],
                ring_send.at[color, inner],
                ring_recv.at[color, inner],
            )
            for color, axis in enumerate(("row_0", "row_1"))
        ]
        for inner in range(2)
    ]
    flat = rings[0] + rings[1]
    group = functools.partial(
        insert_group,
        operators=operators, second=second, first=first, middles=(middle0, middle1), volume=volume,
    )
    group(0)
    pl.semaphore_wait(barrier, 30)
    gathered[half, z, in_plane] = info_ref[...]
    info_copies = exchange(
        plane_peers, lambda peer: info_ref, gathered.at[half, z, in_plane], small_send.at[0], small_recv.at[0]
    )
    pending = list(info_copies)
    for ring in flat:
        ring.send_far()
    group(1)
    for ring in flat:
        ring.send_right()
    group(2)
    for ring in flat:
        ring.send_left()
    group(3)
    for ring in flat:
        ring.forward()
    arrived(info_copies)
    info_copies = exchange(
        line_peers, lambda peer: gathered.at[half, z], gathered.at[half, z], small_send.at[1], small_recv.at[1]
    )
    pending += info_copies

    own_plane = in_plane * 4 + half * 2
    spreads = []
    for inner in range(2):
        spreads.append([])
        for color, axis in enumerate(("row_1", "row_0")):
            rings[inner][color].finish(part.at[color, inner])
            me = lax.axis_index(axis)
            spreads[inner] += exchange(
                others(axis),
                lambda peer, axis=axis, color=color, inner=inner: part.at[color, inner, peer[axis]],
                spread_buffer.at[color, inner, me],
                spread_send.at[color, inner],
                spread_recv.at[color, inner],
            )
    plane_copies = []
    for inner in range(2):
        arrived(spreads[inner])
        pending += spreads[inner]
        for color, axis in enumerate(("row_1", "row_0")):
            me = lax.axis_index(axis)
            total = part[color, inner, me]
            for step in range(1, 4):
                total = total + spread_buffer[color, inner, (me + step) % 4]
            slab[color, inner] = total
        plane_copies += exchange(
            line_peers,
            lambda peer, inner=inner: slab.at[
                peer["half"], inner, pl.ds(pl.multiple_of(peer["col"] * 8, 8), 8)
            ],
            planes.at[half, inner, z],
            plane_send.at[inner],
            plane_recv.at[inner],
        )
        planes[half, inner, z] = slab[half, inner, pl.ds(pl.multiple_of(z * 8, 8), 8)]
        if inner == 0:
            arrived(info_copies)
            bin_counts([gathered[index].reshape(128, 128) for index in range(2)], count_ref)
            insert_counts(table, count_ref, first_ref, second_ref)
        else:
            weight_sums(own_plane, z, table, first_ref, second_ref, weight_ref)
    arrived(plane_copies)
    pending += plane_copies

    maps = [[], []]
    for which in range(2):
        for inner in range(2):
            total = planes[which, inner, 0]
            for index in range(1, 8):
                total = total + planes[which, inner, index]
            maps[which].append(total / (weight_ref[which, inner] + 1.0))
            own[which, inner] = maps[which][inner]
    partner = remote(
        own.at[1 - half], other, small_send.at[4, 0], small_recv.at[4, 0], {"half": 1 - half}
    )
    everyone = others("half", "row_0", "row_1", "col")
    me = (in_plane * 8 + z) * 2 + half
    stat_all[me] = shell_rows(maps[0], maps[1], own_plane, z)
    copies = [
        remote(stat_all.at[me], stat_all.at[me], stat_sem.at[0], stat_sem.at[1], peer) for peer in everyone
    ]
    partner.wait_recv()
    for inner in range(2):
        swap[half * 2 + inner] = own[half, inner]
        swap[(1 - half) * 2 + inner] = other[inner]
    low = iota((4, 128), 1) < 64
    for plane in range(4):
        even = swap[plane, pl.ds(0, 4, stride=2), :]
        odd = swap[plane, pl.ds(1, 4, stride=2), :]
        parts = (
            jnp.where(low, even, pltpu.roll(odd, 64, 1)),
            jnp.where(low, pltpu.roll(even, 64, 1), odd),
        )
        for component in range(2):
            for piece in range(4):
                map_ref[0, component, pl.ds(plane, 1), pl.ds(128 * piece, 128)] = parts[component][
                    piece : piece + 1
                ]
    whole = stat_all.at[pl.ds(0, len(copies))]
    pltpu.make_async_copy(whole, whole, stat_sem.at[1]).wait()
    totals = [stat_all[index] for index in range(8)]
    for index in range(8, 256):
        totals[index % 8] = totals[index % 8] + stat_all[index]
    while len(totals) > 1:
        totals = [first + second for first, second in zip(totals[::2], totals[1::2])]
    stat = jnp.broadcast_to(totals[0], (8, 128))
    power_first, power_second, counts = (pltpu.roll(stat, 128 - 32 * kind, 1) for kind in (1, 2, 3))
    correlation = stat / jnp.sqrt(power_first * power_second + 1e-06)
    power_ref[pl.ds(0, 1), :] = (power_first / counts)[:1, :SHELLS]
    power_ref[pl.ds(1, 1), :] = (power_second / counts)[:1, :SHELLS]
    correlation_ref[...] = correlation[:1, :SHELLS]
    for ring in flat:
        pending += ring.copies
    pending.append(partner)
    for copy in pending:
        copy.wait_send()
    pltpu.make_async_copy(whole, whole, stat_sem.at[0]).wait()


def emit_kernel(map_ref, power_ref, correlation_ref, map_out, power_out, correlation_out, sems):
    pairs = ((map_ref, map_out), (power_ref, power_out), (correlation_ref, correlation_out))
    copies = [
        pltpu.make_async_copy(source, target, sems.at[index]) for index, (source, target) in enumerate(pairs)
    ]
    for copy in copies:
        copy.start()
    for copy in copies:
        copy.wait()


def local(particles, orient_bin, tilt_slope, interp_table):
    hbm = pl.BlockSpec(memory_space=pltpu.HBM)
    vmem = pl.BlockSpec(memory_space=pltpu.VMEM)
    dma = pltpu.SemaphoreType.DMA
    f32 = lambda *shape: pltpu.VMEM(shape, F32)
    shapes = (
        jax.ShapeDtypeStruct((1, 2, 4, 512), F32),
        jax.ShapeDtypeStruct((2, SHELLS), F32),
        jax.ShapeDtypeStruct((1, SHELLS), F32),
    )
    results = pl.pallas_call(
        kernel,
        out_shape=tuple(pltpu.VMEM(shape.shape, F32) for shape in shapes),
        in_specs=[hbm] * 4,
        out_specs=(vmem, vmem, vmem),
        scratch_shapes=[
            pltpu.VMEM((2, 2, GRID, GRID * GRID), BF16),
            pltpu.SMEM((2,), jnp.int32),
            pltpu.SMEM((2, 2), jnp.int32),
            pltpu.VMEM((BINS, 3, GRID, GRID), BF16),
            pltpu.VMEM((2, 32, GRID, 256), BF16),
            f32(GRID * STRIDE, 128),
            f32(GRID * STRIDE, 128),
            f32(4, 2, 2, 4, GRID, 128),
            f32(2, 2, 6, 2, GRID, 128),
            f32(2, 2, 4, GRID, 128),
            f32(2, 2, 4, GRID, 128),
            f32(2, 2, GRID, 128),
            f32(2, 2, 8, 8, 128),
            pltpu.VMEM((1, 128), jnp.int32),
            pltpu.VMEM((2, 8, 16, 1, 128), jnp.int32),
            f32(2, 2, 8, 128),
            f32(2, 2, 8, 128),
            f32(2, 8, 128),
            f32(4, 8, 128),
            f32(256, 1, 128),
            f32((GRID + 1) * 2 * BINS, 128),
            f32(2, BINS, GRID, 128),
            f32(GRID, 128),
            dma((5,)),
            dma((2, 2, 6)),
            dma((2, 2, 6)),
            dma((2, 2, 4)),
            dma((2, 2, 4)),
            dma((2, 16)),
            dma((2, 16)),
            dma((5, 16)),
            dma((5, 16)),
            dma((2,)),
        ],
        compiler_params=pltpu.CompilerParams(
            collective_id=0, has_side_effects=True, vmem_limit_bytes=60 * 2**20
        ),
        name="halfmaps",
    )(particles, orient_bin, tilt_slope, interp_table)
    return pl.pallas_call(
        emit_kernel,
        out_shape=shapes,
        in_specs=[vmem] * 3,
        out_specs=(hbm,) * 3,
        scratch_shapes=[dma((3,))],
        compiler_params=pltpu.CompilerParams(vmem_limit_bytes=2**20),
        name="emit",
    )(*results)


def solution(mesh):
    torus = Mesh(
        mesh.devices.reshape(mesh.shape["half"], 4, 4, mesh.shape["col"]), HALF_ROW_COL
    )
    in_specs = (P(HALF_ROW_COL, None, None, None), P(HALF_ROW_COL), P(HALF_ROW_COL, None), P())
    out_specs = (P("half", None, ("row_0", "row_1"), "col"), P(), P("half", None))
    return jax.shard_map(local, mesh=torus, in_specs=in_specs, out_specs=out_specs, check_vma=False)
```

```python
import functools
import itertools

import jax
import jax.numpy as jnp
from jax import lax
from jax.experimental import pallas as pl
from jax.experimental.pallas import tpu as pltpu
from jax.sharding import Mesh
from jax.sharding import PartitionSpec as P

SHELLS = 29
GRID = 64
BINS = 16
STRIDE = 24
SIZES = {"half": 2, "row_0": 4, "row_1": 4, "col": 8}
HALF_ROW_COL = ("half", "row_0", "row_1", "col")
MESH = pl.DeviceIdType.MESH
F32 = jnp.float32
BF16 = jnp.bfloat16


def iota(shape, dim):
    return lax.broadcasted_iota(jnp.int32, shape, dim)


def owner_rows(x, y):
    index = iota((GRID, GRID), 0)
    group, color, other, inner = index // 16, (index // 8) % 2, (index // 2) % 4, index % 2
    shift = jnp.where(group == 0, 2, jnp.where(group == 1, 1, jnp.where(group == 2, 3, 0)))
    main = (jnp.where(color == 0, x, y) + shift) % 4
    plane = jnp.where(color == 0, 16 * main + 4 * other, 16 * other + 4 * main + 2) + inner
    return (plane == iota((GRID, GRID), 1)).astype(F32).astype(BF16)


def along_first(particle, order, bins, slopes, data, table, first):
    wave_first = iota((GRID, 128), 0) - 32
    wave_third = (iota((GRID, 128), 1) & 63) - 32
    limit = jnp.where(wave_first * wave_third >= 0, slopes[particle, 0], slopes[particle, 1])
    inside = 16 * jnp.abs(wave_third) <= limit * jnp.abs(wave_first)
    weight = inside.astype(F32).astype(BF16)
    kernel = jnp.dot(order, table[bins[particle], 0], preferred_element_type=F32).astype(BF16)

    def pairs(step, carry):
        for inner in range(16):
            pair = step * 16 + inner
            columns = pl.ds(pl.multiple_of(pair * 128, 128), 128)
            both = jnp.concatenate([data[particle, part, :, columns] * weight for part in range(2)], axis=1)
            first[particle, pair] = jnp.dot(kernel, both, preferred_element_type=F32).astype(BF16)
        return carry

    lax.fori_loop(0, 2, pairs, 0)


def third_operator(kernel):
    block_row = iota((256, 256), 0) // 64
    block_col = iota((256, 256), 1) // 64
    matching = (block_row // 2 == block_col % 2) & (block_row % 2 == block_col // 2)
    third = jnp.transpose(kernel.astype(F32))
    third = jnp.concatenate([third, third], axis=1)
    third = jnp.concatenate([third, third], axis=1)
    third = jnp.concatenate([third, third, third, third], axis=0)
    return jnp.where(matching, third, 0.0).astype(BF16)


def insert_group(group, operators, second, first, middles, volume):
    rows = pl.ds(16 * group, 16)
    for particle, middle in enumerate(middles):
        lines = first[particle, :, rows, :].reshape(512, 256)
        lines = jnp.dot(lines, operators[particle], preferred_element_type=F32)
        for pair in range(32):
            middle[pl.ds(2 * pair * STRIDE, 16), :] = lines[16 * pair : 16 * pair + 16, :128]
            middle[pl.ds((2 * pair + 1) * STRIDE, 16), :] = lines[16 * pair : 16 * pair + 16, 128:]
    for place in range(8):
        planes = []
        for inner in range(2):
            sides = [middle[pl.ds(2 * place + inner, GRID, stride=STRIDE), :] for middle in middles]
            planes.append(jnp.concatenate(sides, axis=0).astype(BF16))
        slab = jnp.dot(second, jnp.concatenate(planes, axis=1), preferred_element_type=F32)
        for inner in range(2):
            volume[group, place // 4, inner, place % 4] = slab[:, 128 * inner : 128 * inner + 128]


def bin_counts(infos, count_ref):
    contract = functools.partial(
        lax.dot_general, dimension_numbers=(((1,), (1,)), ((), ())), preferred_element_type=F32
    )
    bin_index = iota((BINS, 128), 0).astype(F32)
    slope_index = iota((GRID, 128), 0).astype(F32)
    parts = [[], []]
    for info in infos:
        fields = jnp.transpose(info.astype(F32))[:8]
        bins = [(fields[particle : particle + 1] == bin_index).astype(F32) for particle in range(2)]
        bins = jnp.concatenate(bins, axis=1).astype(BF16)
        for side in range(2):
            slopes = [
                (fields[2 + 2 * particle + side : 3 + 2 * particle + side] == slope_index).astype(F32)
                for particle in range(2)
            ]
            parts[side].append(contract(bins, jnp.concatenate(slopes, axis=1).astype(BF16)))
    histogram = jnp.concatenate(parts[0] + parts[1], axis=0).astype(BF16)

    reach = (16 * jnp.abs((iota((GRID, 128), 1) & 63) - 32)).astype(F32)
    wave_third = (iota((2 * BINS, 128), 1) & 63) - 32
    nonneg, nonpos = wave_third >= 0, wave_third <= 0

    def counted(distance):
        inside = (reach <= slope_index * distance).astype(F32).astype(BF16)
        counts = jnp.dot(histogram, inside, preferred_element_type=F32)
        return counts[: 2 * BINS], counts[2 * BINS :]

    def place(first):
        return pl.ds(pl.multiple_of(first * 2 * BINS, 2 * BINS), 2 * BINS)

    def planes(step, carry):
        for inner in range(8):
            distance = step * 8 + inner + 1
            same, opposite = counted(distance.astype(F32))
            count_ref[place(32 + distance), :] = jnp.where(nonneg, same, opposite)
            count_ref[place(32 - distance), :] = jnp.where(nonpos, same, opposite)
        return carry

    count_ref[place(32), :] = counted(0.0)[0]
    lax.fori_loop(0, 4, planes, 0)


def insert_counts(table, count_ref, first_ref, second_ref):
    bin_lane = iota((GRID, 128), 1)
    second = jnp.zeros((GRID, 128), F32)
    for which in range(BINS):
        counts = [count_ref[pl.ds(BINS * half + which, GRID, stride=2 * BINS), :] for half in range(2)]
        counts = jnp.concatenate(counts, axis=1).astype(BF16)
        lines = jnp.dot(table[which, 0], counts, preferred_element_type=F32)
        for half in range(2):
            first_ref[half, which] = lines[:, 128 * half : 128 * half + 128]
        total = jnp.sum(table[which, 1].astype(F32), axis=1, keepdims=True)
        second = jnp.where(bin_lane == which, total, second)
    second_ref[...] = second


def weight_sums(plane, col, table, first_ref, second_ref, weight_ref):
    second = second_ref[pl.ds(pl.multiple_of(col * 8, 8), 8), :]
    contract = functools.partial(
        lax.dot_general, dimension_numbers=(((1,), (1,)), ((), ())), preferred_element_type=F32
    )
    sums = [jnp.zeros((8, 128), F32) for _ in range(4)]
    for which in range(BINS):
        first = jnp.concatenate([first_ref[half, which, pl.ds(plane, 2), :] for half in range(2)], axis=0)[:, :GRID]
        high = first.astype(BF16)
        low = (first - high.astype(F32)).astype(BF16)
        third = jnp.concatenate([table[which, 2]] * 2, axis=0)
        lines = contract(high, third) + contract(low, third)
        for index in range(4):
            sums[index] = sums[index] + second[:, which : which + 1] * lines[index : index + 1]
    for index in range(4):
        weight_ref[index // 2, index % 2] = sums[index]


def remote(source, target, send, recv, device):
    copy = pltpu.make_async_remote_copy(
        src_ref=source, dst_ref=target, send_sem=send, recv_sem=recv, device_id=device, device_id_type=MESH
    )
    copy.start()
    return copy


class Ring4:
    def __init__(self, axis, source, buffer, send, recv):
        self.axis, self.source, self.buffer, self.send, self.recv = axis, source, buffer, send, recv
        me = lax.axis_index(axis)
        self.right, self.left = (me + 1) % 4, (me + 3) % 4
        self.copies = [None] * 6

    def copy(self, slot, source, target):
        self.copies[slot] = remote(
            source, self.buffer.at[slot], self.send.at[slot], self.recv.at[slot], {self.axis: target}
        )

    def send_far(self):
        self.copy(0, self.source(0, 0), self.right)
        self.copy(3, self.source(0, 1), self.left)

    def send_right(self):
        self.copy(2, self.source(1, 1), self.right)

    def send_left(self):
        self.copy(5, self.source(2, 0), self.left)

    def forward(self):
        self.copies[0].wait_recv()
        self.buffer[0] = self.buffer[0] + self.source(1, 0)[...]
        self.copy(1, self.buffer.at[0], self.right)
        self.copies[3].wait_recv()
        self.buffer[3] = self.buffer[3] + self.source(2, 1)[...]
        self.copy(4, self.buffer.at[3], self.left)

    def finish(self, result):
        for half, near, other in ((0, 1, 5), (1, 4, 2)):
            self.copies[other].wait_recv()
            self.copies[near].wait_recv()
            result[pl.ds(2 * half, 2)] = (
                self.source(3, half)[...] + self.buffer[near] + self.buffer[other]
            )


def hops(offset, sizes):
    return sum(min(step, size - step) for step, size in zip(offset, sizes))


def others(*axes):
    sizes = [SIZES[axis] for axis in axes]
    offsets = [offset for offset in itertools.product(*map(range, sizes)) if any(offset)]
    offsets.sort(key=lambda offset: -hops(offset, sizes))
    places = {
        axis: [lax.rem(lax.axis_index(axis) + step, size) for step in range(size)]
        for axis, size in zip(axes, sizes)
    }
    return [{axis: places[axis][step] for axis, step in zip(axes, offset)} for offset in offsets]


def exchange(peers, source, target, send, recv):
    return [
        remote(source(peer), target, send.at[index], recv.at[index], peer) for index, peer in enumerate(peers)
    ]


def arrived(copies):
    for copy in copies:
        copy.wait_recv()


def shell_rows(sums_first, sums_second, plane, col):
    wave_second = iota((8, 128), 0) + col * 8 - 32
    wave_third = (iota((8, 128), 1) & 63) - 32
    rest = wave_second * wave_second + wave_third * wave_third
    radius = []
    for index in range(2):
        wave_first = plane + index - 32
        radius.append(rest + wave_first * wave_first)
    real = iota((8, 128), 1) < 64
    values = [
        [first * second for first, second in zip(sums_first, sums_second)],
        [first * first for first in sums_first],
        [second * second for second in sums_second],
        [jnp.where(real, 1.0, 0.0).astype(F32)] * 2,
    ]
    rows = [[] for _ in range(4)]
    for shell in range(32):
        low = 0 if shell == 0 else (shell + 3) ** 2
        high = (shell + 4) ** 2 if shell < SHELLS else low
        masks = [(r >= low) & (r < high) for r in radius]
        for kind in range(4):
            parts = [jnp.where(m, v, 0.0) for m, v in zip(masks, values[kind])]
            rows[kind].append(jnp.sum(parts[0] + parts[1], axis=0, keepdims=True))
    stacked = jnp.concatenate([row for kind in rows for row in kind], axis=0)
    return lax.dot_general(
        jnp.ones((8, 128), F32),
        stacked,
        dimension_numbers=(((1,), (1,)), ((), ())),
        precision=lax.Precision.HIGHEST,
        preferred_element_type=F32,
    )[:1]


def kernel(
    particle_hbm, bin_hbm, slope_hbm, table_hbm, map_ref, power_ref, correlation_ref,
    data, bins, slopes, table, first, middle0, middle1, volume,
    ring_buffer, part, spread_buffer, slab, planes, info_ref, gathered, weight_ref, own, other, swap, stat_all,
    count_ref, first_ref, second_ref,
    local_sem, ring_send, ring_recv, spread_send, spread_recv, plane_send, plane_recv, small_send, small_recv, stat_sem,
):
    half, x, y, z = (lax.axis_index(name) for name in HALF_ROW_COL)
    in_plane, in_line = x * 4 + y, z * 2 + half
    loads = [
        pltpu.make_async_copy(source, target, local_sem.at[index])
        for index, (source, target) in enumerate(
            (
                (bin_hbm, bins),
                (slope_hbm, slopes),
                (table_hbm, table),
                (particle_hbm.at[0], data.at[0]),
                (particle_hbm.at[1], data.at[1]),
            )
        )
    ]
    for load in loads:
        load.start()
    plane_peers, line_peers = others("row_0", "row_1"), others("col", "half")
    barrier = pltpu.get_barrier_semaphore()
    for peer in plane_peers + line_peers:
        pl.semaphore_signal(barrier, inc=1, device_id=peer, device_id_type=MESH)
    loads[0].wait()
    loads[1].wait()
    lane = iota((1, 128), 1)
    info = jnp.zeros((1, 128), jnp.int32)
    for particle in range(2):
        info = jnp.where(lane == particle, bins[particle], info)
        for side in range(2):
            info = jnp.where(lane == 2 + 2 * particle + side, slopes[particle, side], info)
    info_ref[...] = info

    order = owner_rows(x, y)
    loads[2].wait()
    operators = [third_operator(table[bins[particle], 2]) for particle in range(2)]
    second = jnp.concatenate(
        [table[bins[particle], 1].astype(F32) for particle in range(2)], axis=1
    ).astype(BF16)
    for particle in range(2):
        loads[3 + particle].wait()
        along_first(particle, order, bins, slopes, data, table, first)

    rings = [
        [
            Ring4(
                axis,
                lambda group, side, color=color, inner=inner: volume.at[group, color, inner, pl.ds(2 * side, 2)],
                ring_buffer.at[color, inner],
                ring_send.at[color, inner],
                ring_recv.at[color, inner],
            )
            for color, axis in enumerate(("row_0", "row_1"))
        ]
        for inner in range(2)
    ]
    flat = rings[0] + rings[1]
    group = functools.partial(
        insert_group,
        operators=operators, second=second, first=first, middles=(middle0, middle1), volume=volume,
    )
    group(0)
    pl.semaphore_wait(barrier, 30)
    gathered[half, z, in_plane] = info_ref[...]
    info_copies = exchange(
        plane_peers, lambda peer: info_ref, gathered.at[half, z, in_plane], small_send.at[0], small_recv.at[0]
    )
    pending = list(info_copies)
    for ring in flat:
        ring.send_far()
    group(1)
    for ring in flat:
        ring.send_right()
    group(2)
    for ring in flat:
        ring.send_left()
    group(3)
    for ring in flat:
        ring.forward()
    arrived(info_copies)
    info_copies = exchange(
        line_peers, lambda peer: gathered.at[half, z], gathered.at[half, z], small_send.at[1], small_recv.at[1]
    )
    pending += info_copies

    own_plane = in_plane * 4 + half * 2
    spreads = []
    for inner in range(2):
        spreads.append([])
        for color, axis in enumerate(("row_1", "row_0")):
            rings[inner][color].finish(part.at[color, inner])
            me = lax.axis_index(axis)
            spreads[inner] += exchange(
                others(axis),
                lambda peer, axis=axis, color=color, inner=inner: part.at[color, inner, peer[axis]],
                spread_buffer.at[color, inner, me],
                spread_send.at[color, inner],
                spread_recv.at[color, inner],
            )
    plane_copies = []
    for inner in range(2):
        arrived(spreads[inner])
        pending += spreads[inner]
        for color, axis in enumerate(("row_1", "row_0")):
            me = lax.axis_index(axis)
            total = part[color, inner, me]
            for step in range(1, 4):
                total = total + spread_buffer[color, inner, (me + step) % 4]
            slab[color, inner] = total
    plane_copies = exchange(
        line_peers,
        lambda peer: slab.at[peer["half"], :, pl.ds(pl.multiple_of(peer["col"] * 8, 8), 8)],
        planes.at[half, z],
        plane_send.at[0],
        plane_recv.at[0],
    )
    planes[half, z] = slab[half, :, pl.ds(pl.multiple_of(z * 8, 8), 8)]
    arrived(info_copies)
    bin_counts([gathered[index].reshape(128, 128) for index in range(2)], count_ref)
    insert_counts(table, count_ref, first_ref, second_ref)
    weight_sums(own_plane, z, table, first_ref, second_ref, weight_ref)
    arrived(plane_copies)
    pending += plane_copies

    maps = [[], []]
    for which in range(2):
        for inner in range(2):
            total = planes[which, 0, inner]
            for index in range(1, 8):
                total = total + planes[which, index, inner]
            maps[which].append(total / (weight_ref[which, inner] + 1.0))
            own[which, inner] = maps[which][inner]
    partner = remote(
        own.at[1 - half], other, small_send.at[4, 0], small_recv.at[4, 0], {"half": 1 - half}
    )
    everyone = others("half", "row_0", "row_1", "col")
    me = (in_plane * 8 + z) * 2 + half
    stat_all[me] = shell_rows(maps[0], maps[1], own_plane, z)
    copies = [
        remote(stat_all.at[me], stat_all.at[me], stat_sem.at[0], stat_sem.at[1], peer) for peer in everyone
    ]
    partner.wait_recv()
    for inner in range(2):
        swap[half * 2 + inner] = own[half, inner]
        swap[(1 - half) * 2 + inner] = other[inner]
    low = iota((4, 128), 1) < 64
    for plane in range(4):
        even = swap[plane, pl.ds(0, 4, stride=2), :]
        odd = swap[plane, pl.ds(1, 4, stride=2), :]
        parts = (
            jnp.where(low, even, pltpu.roll(odd, 64, 1)),
            jnp.where(low, pltpu.roll(even, 64, 1), odd),
        )
        for component in range(2):
            for piece in range(4):
                map_ref[0, component, pl.ds(plane, 1), pl.ds(128 * piece, 128)] = parts[component][
                    piece : piece + 1
                ]
    for ring in flat:
        pending += ring.copies
    pending.append(partner)
    for copy in pending:
        copy.wait_send()
    whole = stat_all.at[pl.ds(0, len(copies))]
    pltpu.make_async_copy(whole, whole, stat_sem.at[1]).wait()
    totals = [stat_all[index] for index in range(8)]
    for index in range(8, 256):
        totals[index % 8] = totals[index % 8] + stat_all[index]
    while len(totals) > 1:
        totals = [first + second for first, second in zip(totals[::2], totals[1::2])]
    stat = jnp.broadcast_to(totals[0], (8, 128))
    power_first, power_second, counts = (pltpu.roll(stat, 128 - 32 * kind, 1) for kind in (1, 2, 3))
    correlation = stat / jnp.sqrt(power_first * power_second + 1e-06)
    power_ref[pl.ds(0, 1), :] = (power_first / counts)[:1, :SHELLS]
    power_ref[pl.ds(1, 1), :] = (power_second / counts)[:1, :SHELLS]
    correlation_ref[...] = correlation[:1, :SHELLS]
    pltpu.make_async_copy(whole, whole, stat_sem.at[0]).wait()


def emit_kernel(map_ref, power_ref, correlation_ref, map_out, power_out, correlation_out, sems):
    pairs = ((map_ref, map_out), (power_ref, power_out), (correlation_ref, correlation_out))
    copies = [
        pltpu.make_async_copy(source, target, sems.at[index]) for index, (source, target) in enumerate(pairs)
    ]
    for copy in copies:
        copy.start()
    for copy in copies:
        copy.wait()


def local(particles, orient_bin, tilt_slope, interp_table):
    hbm = pl.BlockSpec(memory_space=pltpu.HBM)
    vmem = pl.BlockSpec(memory_space=pltpu.VMEM)
    dma = pltpu.SemaphoreType.DMA
    f32 = lambda *shape: pltpu.VMEM(shape, F32)
    shapes = (
        jax.ShapeDtypeStruct((1, 2, 4, 512), F32),
        jax.ShapeDtypeStruct((2, SHELLS), F32),
        jax.ShapeDtypeStruct((1, SHELLS), F32),
    )
    results = pl.pallas_call(
        kernel,
        out_shape=tuple(pltpu.VMEM(shape.shape, F32) for shape in shapes),
        in_specs=[hbm] * 4,
        out_specs=(vmem, vmem, vmem),
        scratch_shapes=[
            pltpu.VMEM((2, 2, GRID, GRID * GRID), BF16),
            pltpu.SMEM((2,), jnp.int32),
            pltpu.SMEM((2, 2), jnp.int32),
            pltpu.VMEM((BINS, 3, GRID, GRID), BF16),
            pltpu.VMEM((2, 32, GRID, 256), BF16),
            f32(GRID * STRIDE, 128),
            f32(GRID * STRIDE, 128),
            f32(4, 2, 2, 4, GRID, 128),
            f32(2, 2, 6, 2, GRID, 128),
            f32(2, 2, 4, GRID, 128),
            f32(2, 2, 4, GRID, 128),
            f32(2, 2, GRID, 128),
            f32(2, 8, 2, 8, 128),
            pltpu.VMEM((1, 128), jnp.int32),
            pltpu.VMEM((2, 8, 16, 1, 128), jnp.int32),
            f32(2, 2, 8, 128),
            f32(2, 2, 8, 128),
            f32(2, 8, 128),
            f32(4, 8, 128),
            f32(256, 1, 128),
            f32((GRID + 1) * 2 * BINS, 128),
            f32(2, BINS, GRID, 128),
            f32(GRID, 128),
            dma((5,)),
            dma((2, 2, 6)),
            dma((2, 2, 6)),
            dma((2, 2, 4)),
            dma((2, 2, 4)),
            dma((2, 16)),
            dma((2, 16)),
            dma((5, 16)),
            dma((5, 16)),
            dma((2,)),
        ],
        compiler_params=pltpu.CompilerParams(
            collective_id=0, has_side_effects=True, vmem_limit_bytes=60 * 2**20
        ),
        name="halfmaps",
    )(particles, orient_bin, tilt_slope, interp_table)
    return pl.pallas_call(
        emit_kernel,
        out_shape=shapes,
        in_specs=[vmem] * 3,
        out_specs=(hbm,) * 3,
        scratch_shapes=[dma((3,))],
        compiler_params=pltpu.CompilerParams(vmem_limit_bytes=2**20),
        name="emit",
    )(*results)


def solution(mesh):
    torus = Mesh(
        mesh.devices.reshape(mesh.shape["half"], 4, 4, mesh.shape["col"]), HALF_ROW_COL
    )
    in_specs = (P(HALF_ROW_COL, None, None, None), P(HALF_ROW_COL), P(HALF_ROW_COL, None), P())
    out_specs = (P("half", None, ("row_0", "row_1"), "col"), P(), P("half", None))
    return jax.shard_map(local, mesh=torus, in_specs=in_specs, out_specs=out_specs, check_vma=False)
```

```python
import functools
import itertools

import jax
import jax.numpy as jnp
from jax import lax
from jax.experimental import pallas as pl
from jax.experimental.pallas import tpu as pltpu
from jax.sharding import Mesh
from jax.sharding import PartitionSpec as P

SHELLS = 29
GRID = 64
BINS = 16
STRIDE = 24
SIZES = {"half": 2, "row_0": 4, "row_1": 4, "col": 8}
HALF_ROW_COL = ("half", "row_0", "row_1", "col")
MESH = pl.DeviceIdType.MESH
F32 = jnp.float32
BF16 = jnp.bfloat16


def iota(shape, dim):
    return lax.broadcasted_iota(jnp.int32, shape, dim)


def owner_rows(x, y):
    index = iota((GRID, GRID), 0)
    group, color, other, inner = index // 16, (index // 8) % 2, (index // 2) % 4, index % 2
    shift = jnp.where(group == 0, 2, jnp.where(group == 1, 1, jnp.where(group == 2, 3, 0)))
    main = (jnp.where(color == 0, x, y) + shift) % 4
    plane = jnp.where(color == 0, 16 * main + 4 * other, 16 * other + 4 * main + 2) + inner
    return (plane == iota((GRID, GRID), 1)).astype(F32).astype(BF16)


def along_first(particle, order, bins, slopes, data, table, first):
    wave_first = iota((GRID, 128), 0) - 32
    wave_third = (iota((GRID, 128), 1) & 63) - 32
    limit = jnp.where(wave_first * wave_third >= 0, slopes[particle, 0], slopes[particle, 1])
    inside = 16 * jnp.abs(wave_third) <= limit * jnp.abs(wave_first)
    weight = inside.astype(F32).astype(BF16)
    kernel = jnp.dot(order, table[bins[particle], 0], preferred_element_type=F32).astype(BF16)

    def pairs(step, carry):
        for inner in range(16):
            pair = step * 16 + inner
            columns = pl.ds(pl.multiple_of(pair * 128, 128), 128)
            both = jnp.concatenate([data[particle, part, :, columns] * weight for part in range(2)], axis=1)
            first[particle, pair] = jnp.dot(kernel, both, preferred_element_type=F32).astype(BF16)
        return carry

    lax.fori_loop(0, 2, pairs, 0)


def third_operator(kernel):
    block_row = iota((256, 256), 0) // 64
    block_col = iota((256, 256), 1) // 64
    matching = (block_row // 2 == block_col % 2) & (block_row % 2 == block_col // 2)
    third = jnp.transpose(kernel.astype(F32))
    third = jnp.concatenate([third, third], axis=1)
    third = jnp.concatenate([third, third], axis=1)
    third = jnp.concatenate([third, third, third, third], axis=0)
    return jnp.where(matching, third, 0.0).astype(BF16)


def insert_group(group, operators, second, first, middles, volume):
    rows = pl.ds(16 * group, 16)
    for particle, middle in enumerate(middles):
        lines = first[particle, :, rows, :].reshape(512, 256)
        lines = jnp.dot(lines, operators[particle], preferred_element_type=F32)
        for pair in range(32):
            middle[pl.ds(2 * pair * STRIDE, 16), :] = lines[16 * pair : 16 * pair + 16, :128]
            middle[pl.ds((2 * pair + 1) * STRIDE, 16), :] = lines[16 * pair : 16 * pair + 16, 128:]
    for place in range(8):
        planes = []
        for inner in range(2):
            sides = [middle[pl.ds(2 * place + inner, GRID, stride=STRIDE), :] for middle in middles]
            planes.append(jnp.concatenate(sides, axis=0).astype(BF16))
        slab = jnp.dot(second, jnp.concatenate(planes, axis=1), preferred_element_type=F32)
        for inner in range(2):
            volume[group, place // 4, inner, place % 4] = slab[:, 128 * inner : 128 * inner + 128]


def bin_counts(infos, count_ref):
    contract = functools.partial(
        lax.dot_general, dimension_numbers=(((1,), (1,)), ((), ())), preferred_element_type=F32
    )
    bin_index = iota((BINS, 128), 0).astype(F32)
    slope_index = iota((GRID, 128), 0).astype(F32)
    parts = [[], []]
    for info in infos:
        fields = jnp.transpose(info.astype(F32))[:8]
        bins = [(fields[particle : particle + 1] == bin_index).astype(F32) for particle in range(2)]
        bins = jnp.concatenate(bins, axis=1).astype(BF16)
        for side in range(2):
            slopes = [
                (fields[2 + 2 * particle + side : 3 + 2 * particle + side] == slope_index).astype(F32)
                for particle in range(2)
            ]
            parts[side].append(contract(bins, jnp.concatenate(slopes, axis=1).astype(BF16)))
    histogram = jnp.concatenate(parts[0] + parts[1], axis=0).astype(BF16)

    reach = (16 * jnp.abs((iota((GRID, 128), 1) & 63) - 32)).astype(F32)
    wave_third = (iota((2 * BINS, 128), 1) & 63) - 32
    nonneg, nonpos = wave_third >= 0, wave_third <= 0

    def counted(distance):
        inside = (reach <= slope_index * distance).astype(F32).astype(BF16)
        counts = jnp.dot(histogram, inside, preferred_element_type=F32)
        return counts[: 2 * BINS], counts[2 * BINS :]

    def place(first):
        return pl.ds(pl.multiple_of(first * 2 * BINS, 2 * BINS), 2 * BINS)

    def planes(step, carry):
        for inner in range(8):
            distance = step * 8 + inner + 1
            same, opposite = counted(distance.astype(F32))
            count_ref[place(32 + distance), :] = jnp.where(nonneg, same, opposite)
            count_ref[place(32 - distance), :] = jnp.where(nonpos, same, opposite)
        return carry

    count_ref[place(32), :] = counted(0.0)[0]
    lax.fori_loop(0, 4, planes, 0)


def insert_counts(table, count_ref, first_ref, second_ref):
    bin_lane = iota((GRID, 128), 1)
    second = jnp.zeros((GRID, 128), F32)
    for which in range(BINS):
        counts = [count_ref[pl.ds(BINS * half + which, GRID, stride=2 * BINS), :] for half in range(2)]
        counts = jnp.concatenate(counts, axis=1).astype(BF16)
        lines = jnp.dot(table[which, 0], counts, preferred_element_type=F32)
        for half in range(2):
            first_ref[half, which] = lines[:, 128 * half : 128 * half + 128]
        total = jnp.sum(table[which, 1].astype(F32), axis=1, keepdims=True)
        second = jnp.where(bin_lane == which, total, second)
    second_ref[...] = second


def weight_sums(plane, col, table, first_ref, second_ref, weight_ref):
    second = second_ref[pl.ds(pl.multiple_of(col * 8, 8), 8), :]
    contract = functools.partial(
        lax.dot_general, dimension_numbers=(((1,), (1,)), ((), ())), preferred_element_type=F32
    )
    sums = [jnp.zeros((8, 128), F32) for _ in range(4)]
    for which in range(BINS):
        first = jnp.concatenate([first_ref[half, which, pl.ds(plane, 2), :] for half in range(2)], axis=0)[:, :GRID]
        high = first.astype(BF16)
        low = (first - high.astype(F32)).astype(BF16)
        third = jnp.concatenate([table[which, 2]] * 2, axis=0)
        lines = contract(high, third) + contract(low, third)
        for index in range(4):
            sums[index] = sums[index] + second[:, which : which + 1] * lines[index : index + 1]
    for index in range(4):
        weight_ref[index // 2, index % 2] = sums[index]


def remote(source, target, send, recv, device):
    copy = pltpu.make_async_remote_copy(
        src_ref=source, dst_ref=target, send_sem=send, recv_sem=recv, device_id=device, device_id_type=MESH
    )
    copy.start()
    return copy


class Ring4:
    def __init__(self, axis, source, buffer, send, recv):
        self.axis, self.source, self.buffer, self.send, self.recv = axis, source, buffer, send, recv
        me = lax.axis_index(axis)
        self.right, self.left = (me + 1) % 4, (me + 3) % 4
        self.copies = [None] * 6

    def copy(self, slot, source, target):
        self.copies[slot] = remote(
            source, self.buffer.at[slot], self.send.at[slot], self.recv.at[slot], {self.axis: target}
        )

    def send_far(self):
        self.copy(0, self.source(0, 0), self.right)
        self.copy(3, self.source(0, 1), self.left)

    def send_right(self):
        self.copy(2, self.source(1, 1), self.right)

    def send_left(self):
        self.copy(5, self.source(2, 0), self.left)

    def forward(self):
        self.copies[0].wait_recv()
        self.buffer[0] = self.buffer[0] + self.source(1, 0)[...]
        self.copy(1, self.buffer.at[0], self.right)
        self.copies[3].wait_recv()
        self.buffer[3] = self.buffer[3] + self.source(2, 1)[...]
        self.copy(4, self.buffer.at[3], self.left)

    def finish(self, result):
        for half, near, other in ((0, 1, 5), (1, 4, 2)):
            self.copies[other].wait_recv()
            self.copies[near].wait_recv()
            result[pl.ds(2 * half, 2)] = (
                self.source(3, half)[...] + self.buffer[near] + self.buffer[other]
            )


def hops(offset, sizes):
    return sum(min(step, size - step) for step, size in zip(offset, sizes))


def others(*axes):
    sizes = [SIZES[axis] for axis in axes]
    offsets = [offset for offset in itertools.product(*map(range, sizes)) if any(offset)]
    offsets.sort(key=lambda offset: -hops(offset, sizes))
    places = {
        axis: [lax.rem(lax.axis_index(axis) + step, size) for step in range(size)]
        for axis, size in zip(axes, sizes)
    }
    return [{axis: places[axis][step] for axis, step in zip(axes, offset)} for offset in offsets]


def exchange(peers, source, target, send, recv):
    return [
        remote(source(peer), target, send.at[index], recv.at[index], peer) for index, peer in enumerate(peers)
    ]


def arrived(copies):
    for copy in copies:
        copy.wait_recv()


def shell_rows(sums_first, sums_second, plane, col):
    wave_second = iota((8, 128), 0) + col * 8 - 32
    wave_third = (iota((8, 128), 1) & 63) - 32
    rest = wave_second * wave_second + wave_third * wave_third
    radius = []
    for index in range(2):
        wave_first = plane + index - 32
        radius.append(rest + wave_first * wave_first)
    real = iota((8, 128), 1) < 64
    values = [
        [first * second for first, second in zip(sums_first, sums_second)],
        [first * first for first in sums_first],
        [second * second for second in sums_second],
        [jnp.where(real, 1.0, 0.0).astype(F32)] * 2,
    ]
    rows = [[] for _ in range(4)]
    for shell in range(32):
        low = 0 if shell == 0 else (shell + 3) ** 2
        high = (shell + 4) ** 2 if shell < SHELLS else low
        masks = [(r >= low) & (r < high) for r in radius]
        for kind in range(4):
            parts = [jnp.where(m, v, 0.0) for m, v in zip(masks, values[kind])]
            rows[kind].append(jnp.sum(parts[0] + parts[1], axis=0, keepdims=True))
    stacked = jnp.concatenate([row for kind in rows for row in kind], axis=0)
    return lax.dot_general(
        jnp.ones((8, 128), F32),
        stacked,
        dimension_numbers=(((1,), (1,)), ((), ())),
        precision=lax.Precision.HIGHEST,
        preferred_element_type=F32,
    )[:1]


def kernel(
    particle_hbm, bin_hbm, slope_hbm, table_hbm, map_ref, power_ref, correlation_ref,
    data, bins, slopes, table, first, middle0, middle1, volume,
    ring_buffer, part, spread_buffer, slab, planes, info_ref, gathered, weight_ref, own, other, swap, stat_all,
    count_ref, first_ref, second_ref,
    local_sem, ring_send, ring_recv, spread_send, spread_recv, plane_send, plane_recv, small_send, small_recv, stat_sem, relay_sem,
):
    half, x, y, z = (lax.axis_index(name) for name in HALF_ROW_COL)
    in_plane, in_line = x * 4 + y, z * 2 + half
    loads = [
        pltpu.make_async_copy(source, target, local_sem.at[index])
        for index, (source, target) in enumerate(
            (
                (bin_hbm, bins),
                (slope_hbm, slopes),
                (table_hbm, table),
                (particle_hbm.at[0], data.at[0]),
                (particle_hbm.at[1], data.at[1]),
            )
        )
    ]
    for load in loads:
        load.start()
    line_peers = others("col", "half")
    barrier = pltpu.get_barrier_semaphore()
    beside = [{"col": lax.rem(z + step, 8)} for step in (1, 7)]
    near = others("row_0") + others("row_1") + beside + others("half")
    for peer in near:
        pl.semaphore_signal(barrier, inc=1, device_id=peer, device_id_type=MESH)
    loads[0].wait()
    loads[1].wait()
    lane = iota((1, 128), 1)
    info = jnp.zeros((1, 128), jnp.int32)
    for particle in range(2):
        info = jnp.where(lane == particle, bins[particle], info)
        for side in range(2):
            info = jnp.where(lane == 2 + 2 * particle + side, slopes[particle, side], info)
    info_ref[...] = info

    order = owner_rows(x, y)
    loads[2].wait()
    operators = [third_operator(table[bins[particle], 2]) for particle in range(2)]
    second = jnp.concatenate(
        [table[bins[particle], 1].astype(F32) for particle in range(2)], axis=1
    ).astype(BF16)
    for particle in range(2):
        loads[3 + particle].wait()
        along_first(particle, order, bins, slopes, data, table, first)

    rings = [
        [
            Ring4(
                axis,
                lambda group, side, color=color, inner=inner: volume.at[group, color, inner, pl.ds(2 * side, 2)],
                ring_buffer.at[color, inner],
                ring_send.at[color, inner],
                ring_recv.at[color, inner],
            )
            for color, axis in enumerate(("row_0", "row_1"))
        ]
        for inner in range(2)
    ]
    flat = rings[0] + rings[1]
    group = functools.partial(
        insert_group,
        operators=operators, second=second, first=first, middles=(middle0, middle1), volume=volume,
    )
    group(0)
    pl.semaphore_wait(barrier, len(near))

    def relay(index, peers):
        for peer in peers:
            pl.semaphore_signal(relay_sem.at[index], inc=1, device_id=peer, device_id_type=MESH)

    relay(0, beside)
    gathered[half, z, x, y] = info_ref[...]
    info_copies = exchange(
        others("row_0"), lambda peer: info_ref, gathered.at[half, z, x, y], small_send.at[0], small_recv.at[0]
    )
    pending = list(info_copies)
    for ring in flat:
        ring.send_far()
    group(1)
    for ring in flat:
        ring.send_right()
    pl.semaphore_wait(relay_sem.at[0], 2)
    relay(1, beside)
    group(2)
    for ring in flat:
        ring.send_left()
    pl.semaphore_wait(relay_sem.at[1], 2)
    relay(2, beside)
    group(3)
    arrived(info_copies)
    column = gathered.at[half, z, :, y]
    info_copies = exchange(others("row_1"), lambda peer: column, column, small_send.at[2], small_recv.at[2])
    pending += info_copies
    pl.semaphore_wait(relay_sem.at[2], 2)
    relay(3, others("half"))
    for ring in flat:
        ring.forward()
    pl.semaphore_wait(relay_sem.at[3], 1)
    arrived(info_copies)
    info_copies = exchange(
        line_peers, lambda peer: gathered.at[half, z], gathered.at[half, z], small_send.at[1], small_recv.at[1]
    )
    pending += info_copies

    own_plane = in_plane * 4 + half * 2
    spreads = []
    for inner in range(2):
        spreads.append([])
        for color, axis in enumerate(("row_1", "row_0")):
            rings[inner][color].finish(part.at[color, inner])
            me = lax.axis_index(axis)
            spreads[inner] += exchange(
                others(axis),
                lambda peer, axis=axis, color=color, inner=inner: part.at[color, inner, peer[axis]],
                spread_buffer.at[color, inner, me],
                spread_send.at[color, inner],
                spread_recv.at[color, inner],
            )
    plane_copies = []
    for inner in range(2):
        arrived(spreads[inner])
        pending += spreads[inner]
        for color, axis in enumerate(("row_1", "row_0")):
            me = lax.axis_index(axis)
            total = part[color, inner, me]
            for step in range(1, 4):
                total = total + spread_buffer[color, inner, (me + step) % 4]
            slab[color, inner] = total
    plane_copies = exchange(
        line_peers,
        lambda peer: slab.at[peer["half"], :, pl.ds(pl.multiple_of(peer["col"] * 8, 8), 8)],
        planes.at[half, z],
        plane_send.at[0],
        plane_recv.at[0],
    )
    planes[half, z] = slab[half, :, pl.ds(pl.multiple_of(z * 8, 8), 8)]
    arrived(info_copies)
    bin_counts([gathered[index].reshape(128, 128) for index in range(2)], count_ref)
    insert_counts(table, count_ref, first_ref, second_ref)
    weight_sums(own_plane, z, table, first_ref, second_ref, weight_ref)
    arrived(plane_copies)
    pending += plane_copies

    maps = [[], []]
    for which in range(2):
        for inner in range(2):
            total = planes[which, 0, inner]
            for index in range(1, 8):
                total = total + planes[which, index, inner]
            maps[which].append(total / (weight_ref[which, inner] + 1.0))
            own[which, inner] = maps[which][inner]
    partner = remote(
        own.at[1 - half], other, small_send.at[4, 0], small_recv.at[4, 0], {"half": 1 - half}
    )
    everyone = others("half", "row_0", "row_1", "col")
    me = (in_plane * 8 + z) * 2 + half
    stat_all[me] = shell_rows(maps[0], maps[1], own_plane, z)
    copies = [
        remote(stat_all.at[me], stat_all.at[me], stat_sem.at[0], stat_sem.at[1], peer) for peer in everyone
    ]
    partner.wait_recv()
    for inner in range(2):
        swap[half * 2 + inner] = own[half, inner]
        swap[(1 - half) * 2 + inner] = other[inner]
    low = iota((4, 128), 1) < 64
    for plane in range(4):
        even = swap[plane, pl.ds(0, 4, stride=2), :]
        odd = swap[plane, pl.ds(1, 4, stride=2), :]
        parts = (
            jnp.where(low, even, pltpu.roll(odd, 64, 1)),
            jnp.where(low, pltpu.roll(even, 64, 1), odd),
        )
        for component in range(2):
            for piece in range(4):
                map_ref[0, component, pl.ds(plane, 1), pl.ds(128 * piece, 128)] = parts[component][
                    piece : piece + 1
                ]
    for ring in flat:
        pending += ring.copies
    pending.append(partner)
    for copy in pending:
        copy.wait_send()
    whole = stat_all.at[pl.ds(0, len(copies))]
    pltpu.make_async_copy(whole, whole, stat_sem.at[1]).wait()
    totals = [stat_all[index] for index in range(8)]
    for index in range(8, 256):
        totals[index % 8] = totals[index % 8] + stat_all[index]
    while len(totals) > 1:
        totals = [first + second for first, second in zip(totals[::2], totals[1::2])]
    stat = jnp.broadcast_to(totals[0], (8, 128))
    power_first, power_second, counts = (pltpu.roll(stat, 128 - 32 * kind, 1) for kind in (1, 2, 3))
    correlation = stat / jnp.sqrt(power_first * power_second + 1e-06)
    power_ref[pl.ds(0, 1), :] = (power_first / counts)[:1, :SHELLS]
    power_ref[pl.ds(1, 1), :] = (power_second / counts)[:1, :SHELLS]
    correlation_ref[...] = correlation[:1, :SHELLS]
    pltpu.make_async_copy(whole, whole, stat_sem.at[0]).wait()


def emit_kernel(map_ref, power_ref, correlation_ref, map_out, power_out, correlation_out, sems):
    pairs = ((map_ref, map_out), (power_ref, power_out), (correlation_ref, correlation_out))
    copies = [
        pltpu.make_async_copy(source, target, sems.at[index]) for index, (source, target) in enumerate(pairs)
    ]
    for copy in copies:
        copy.start()
    for copy in copies:
        copy.wait()


def local(particles, orient_bin, tilt_slope, interp_table):
    hbm = pl.BlockSpec(memory_space=pltpu.HBM)
    vmem = pl.BlockSpec(memory_space=pltpu.VMEM)
    dma = pltpu.SemaphoreType.DMA
    f32 = lambda *shape: pltpu.VMEM(shape, F32)
    shapes = (
        jax.ShapeDtypeStruct((1, 2, 4, 512), F32),
        jax.ShapeDtypeStruct((2, SHELLS), F32),
        jax.ShapeDtypeStruct((1, SHELLS), F32),
    )
    results = pl.pallas_call(
        kernel,
        out_shape=tuple(pltpu.VMEM(shape.shape, F32) for shape in shapes),
        in_specs=[hbm] * 4,
        out_specs=(vmem, vmem, vmem),
        scratch_shapes=[
            pltpu.VMEM((2, 2, GRID, GRID * GRID), BF16),
            pltpu.SMEM((2,), jnp.int32),
            pltpu.SMEM((2, 2), jnp.int32),
            pltpu.VMEM((BINS, 3, GRID, GRID), BF16),
            pltpu.VMEM((2, 32, GRID, 256), BF16),
            f32(GRID * STRIDE, 128),
            f32(GRID * STRIDE, 128),
            f32(4, 2, 2, 4, GRID, 128),
            f32(2, 2, 6, 2, GRID, 128),
            f32(2, 2, 4, GRID, 128),
            f32(2, 2, 4, GRID, 128),
            f32(2, 2, GRID, 128),
            f32(2, 8, 2, 8, 128),
            pltpu.VMEM((1, 128), jnp.int32),
            pltpu.VMEM((2, 8, 4, 4, 1, 128), jnp.int32),
            f32(2, 2, 8, 128),
            f32(2, 2, 8, 128),
            f32(2, 8, 128),
            f32(4, 8, 128),
            f32(256, 1, 128),
            f32((GRID + 1) * 2 * BINS, 128),
            f32(2, BINS, GRID, 128),
            f32(GRID, 128),
            dma((5,)),
            dma((2, 2, 6)),
            dma((2, 2, 6)),
            dma((2, 2, 4)),
            dma((2, 2, 4)),
            dma((2, 16)),
            dma((2, 16)),
            dma((5, 16)),
            dma((5, 16)),
            dma((2,)),
            pltpu.SemaphoreType.REGULAR((4,)),
        ],
        compiler_params=pltpu.CompilerParams(
            collective_id=0, has_side_effects=True, vmem_limit_bytes=60 * 2**20
        ),
        name="halfmaps",
    )(particles, orient_bin, tilt_slope, interp_table)
    return pl.pallas_call(
        emit_kernel,
        out_shape=shapes,
        in_specs=[vmem] * 3,
        out_specs=(hbm,) * 3,
        scratch_shapes=[dma((3,))],
        compiler_params=pltpu.CompilerParams(vmem_limit_bytes=2**20),
        name="emit",
    )(*results)


def solution(mesh):
    torus = Mesh(
        mesh.devices.reshape(mesh.shape["half"], 4, 4, mesh.shape["col"]), HALF_ROW_COL
    )
    in_specs = (P(HALF_ROW_COL, None, None, None), P(HALF_ROW_COL), P(HALF_ROW_COL, None), P())
    out_specs = (P("half", None, ("row_0", "row_1"), "col"), P(), P("half", None))
    return jax.shard_map(local, mesh=torus, in_specs=in_specs, out_specs=out_specs, check_vma=False)
```

```python
import functools
import itertools

import jax
import jax.numpy as jnp
from jax import lax
from jax.experimental import pallas as pl
from jax.experimental.pallas import tpu as pltpu
from jax.sharding import Mesh
from jax.sharding import PartitionSpec as P

SHELLS = 29
GRID = 64
BINS = 16
STRIDE = 24
SIZES = {"half": 2, "row_0": 4, "row_1": 4, "col": 8}
HALF_ROW_COL = ("half", "row_0", "row_1", "col")
MESH = pl.DeviceIdType.MESH
F32 = jnp.float32
BF16 = jnp.bfloat16


def iota(shape, dim):
    return lax.broadcasted_iota(jnp.int32, shape, dim)


def owner_rows(x, y):
    index = iota((GRID, GRID), 0)
    group, color, other, inner = index // 16, (index // 8) % 2, (index // 2) % 4, index % 2
    shift = jnp.where(group == 0, 2, jnp.where(group == 1, 1, jnp.where(group == 2, 3, 0)))
    main = (jnp.where(color == 0, x, y) + shift) % 4
    plane = jnp.where(color == 0, 16 * main + 4 * other, 16 * other + 4 * main + 2) + inner
    return (plane == iota((GRID, GRID), 1)).astype(F32).astype(BF16)


def wedge(particle, slopes):
    wave_first = iota((GRID, 128), 0) - 32
    wave_third = (iota((GRID, 128), 1) & 63) - 32
    limit = jnp.where(wave_first * wave_third >= 0, slopes[particle, 0], slopes[particle, 1])
    return (16 * jnp.abs(wave_third) <= limit * jnp.abs(wave_first)).astype(F32).astype(BF16)


def along_first(particle, begin, end, rows, kernel, weight, data, first):
    def pairs(step, carry):
        for inner in range(16):
            pair = begin + step * 16 + inner
            columns = pl.ds(pl.multiple_of(pair * 128, 128), 128)
            both = jnp.concatenate([data[particle, part, :, columns] * weight for part in range(2)], axis=1)
            lines = jnp.dot(kernel, both, preferred_element_type=F32)
            first[particle, pair, rows, :] = lines.astype(BF16)
        return carry

    lax.fori_loop(0, (end - begin) // 16, pairs, 0)


def third_operator(kernel):
    block_row = iota((256, 256), 0) // 64
    block_col = iota((256, 256), 1) // 64
    matching = (block_row // 2 == block_col % 2) & (block_row % 2 == block_col // 2)
    third = jnp.transpose(kernel.astype(F32))
    third = jnp.concatenate([third, third], axis=1)
    third = jnp.concatenate([third, third], axis=1)
    third = jnp.concatenate([third, third, third, third], axis=0)
    return jnp.where(matching, third, 0.0).astype(BF16)


def insert_group(group, operators, second, first, middles, volume):
    rows = pl.ds(16 * group, 16)
    for particle, middle in enumerate(middles):
        lines = first[particle, :, rows, :].reshape(512, 256)
        lines = jnp.dot(lines, operators[particle], preferred_element_type=F32)
        for pair in range(32):
            middle[pl.ds(2 * pair * STRIDE, 16), :] = lines[16 * pair : 16 * pair + 16, :128]
            middle[pl.ds((2 * pair + 1) * STRIDE, 16), :] = lines[16 * pair : 16 * pair + 16, 128:]
    for place in range(8):
        planes = []
        for inner in range(2):
            sides = [middle[pl.ds(2 * place + inner, GRID, stride=STRIDE), :] for middle in middles]
            planes.append(jnp.concatenate(sides, axis=0).astype(BF16))
        slab = jnp.dot(second, jnp.concatenate(planes, axis=1), preferred_element_type=F32)
        for inner in range(2):
            volume[group, place // 4, inner, place % 4] = slab[:, 128 * inner : 128 * inner + 128]


def bin_counts(infos, count_ref):
    contract = functools.partial(
        lax.dot_general, dimension_numbers=(((1,), (1,)), ((), ())), preferred_element_type=F32
    )
    bin_index = iota((BINS, 128), 0).astype(F32)
    slope_index = iota((GRID, 128), 0).astype(F32)
    parts = [[], []]
    for info in infos:
        fields = jnp.transpose(info.astype(F32))[:8]
        bins = [(fields[particle : particle + 1] == bin_index).astype(F32) for particle in range(2)]
        bins = jnp.concatenate(bins, axis=1).astype(BF16)
        for side in range(2):
            slopes = [
                (fields[2 + 2 * particle + side : 3 + 2 * particle + side] == slope_index).astype(F32)
                for particle in range(2)
            ]
            parts[side].append(contract(bins, jnp.concatenate(slopes, axis=1).astype(BF16)))
    histogram = jnp.concatenate(parts[0] + parts[1], axis=0).astype(BF16)

    reach = (16 * jnp.abs((iota((GRID, 128), 1) & 63) - 32)).astype(F32)
    wave_third = (iota((2 * BINS, 128), 1) & 63) - 32
    nonneg, nonpos = wave_third >= 0, wave_third <= 0

    def counted(distance):
        inside = (reach <= slope_index * distance).astype(F32).astype(BF16)
        counts = jnp.dot(histogram, inside, preferred_element_type=F32)
        return counts[: 2 * BINS], counts[2 * BINS :]

    def place(first):
        return pl.ds(pl.multiple_of(first * 2 * BINS, 2 * BINS), 2 * BINS)

    def planes(step, carry):
        for inner in range(8):
            distance = step * 8 + inner + 1
            same, opposite = counted(distance.astype(F32))
            count_ref[place(32 + distance), :] = jnp.where(nonneg, same, opposite)
            count_ref[place(32 - distance), :] = jnp.where(nonpos, same, opposite)
        return carry

    count_ref[place(32), :] = counted(0.0)[0]
    lax.fori_loop(0, 4, planes, 0)


def insert_counts(table, count_ref, first_ref, second_ref):
    bin_lane = iota((GRID, 128), 1)
    second = jnp.zeros((GRID, 128), F32)
    for which in range(BINS):
        counts = [count_ref[pl.ds(BINS * half + which, GRID, stride=2 * BINS), :] for half in range(2)]
        counts = jnp.concatenate(counts, axis=1).astype(BF16)
        lines = jnp.dot(table[which, 0], counts, preferred_element_type=F32)
        for half in range(2):
            first_ref[half, which] = lines[:, 128 * half : 128 * half + 128]
        total = jnp.sum(table[which, 1].astype(F32), axis=1, keepdims=True)
        second = jnp.where(bin_lane == which, total, second)
    second_ref[...] = second


def weight_sums(plane, col, table, first_ref, second_ref, weight_ref):
    second = second_ref[pl.ds(pl.multiple_of(col * 8, 8), 8), :]
    contract = functools.partial(
        lax.dot_general, dimension_numbers=(((1,), (1,)), ((), ())), preferred_element_type=F32
    )
    sums = [jnp.zeros((8, 128), F32) for _ in range(4)]
    for which in range(BINS):
        first = jnp.concatenate([first_ref[half, which, pl.ds(plane, 2), :] for half in range(2)], axis=0)[:, :GRID]
        high = first.astype(BF16)
        low = (first - high.astype(F32)).astype(BF16)
        third = jnp.concatenate([table[which, 2]] * 2, axis=0)
        lines = contract(high, third) + contract(low, third)
        for index in range(4):
            sums[index] = sums[index] + second[:, which : which + 1] * lines[index : index + 1]
    for index in range(4):
        weight_ref[index // 2, index % 2] = sums[index]


def remote(source, target, send, recv, device):
    copy = pltpu.make_async_remote_copy(
        src_ref=source, dst_ref=target, send_sem=send, recv_sem=recv, device_id=device, device_id_type=MESH
    )
    copy.start()
    return copy


class Ring4:
    def __init__(self, axis, source, buffer, send, recv):
        self.axis, self.source, self.buffer, self.send, self.recv = axis, source, buffer, send, recv
        me = lax.axis_index(axis)
        self.right, self.left = (me + 1) % 4, (me + 3) % 4
        self.copies = [None] * 6

    def copy(self, slot, source, target):
        self.copies[slot] = remote(
            source, self.buffer.at[slot], self.send.at[slot], self.recv.at[slot], {self.axis: target}
        )

    def send_far(self):
        self.copy(0, self.source(0, 0), self.right)
        self.copy(3, self.source(0, 1), self.left)

    def send_right(self):
        self.copy(2, self.source(1, 1), self.right)

    def send_left(self):
        self.copy(5, self.source(2, 0), self.left)

    def forward(self):
        self.copies[0].wait_recv()
        self.buffer[0] = self.buffer[0] + self.source(1, 0)[...]
        self.copy(1, self.buffer.at[0], self.right)
        self.copies[3].wait_recv()
        self.buffer[3] = self.buffer[3] + self.source(2, 1)[...]
        self.copy(4, self.buffer.at[3], self.left)

    def finish(self, result):
        for half, near, other in ((0, 1, 5), (1, 4, 2)):
            self.copies[other].wait_recv()
            self.copies[near].wait_recv()
            result[pl.ds(2 * half, 2)] = (
                self.source(3, half)[...] + self.buffer[near] + self.buffer[other]
            )


def hops(offset, sizes):
    return sum(min(step, size - step) for step, size in zip(offset, sizes))


def others(*axes):
    sizes = [SIZES[axis] for axis in axes]
    offsets = [offset for offset in itertools.product(*map(range, sizes)) if any(offset)]
    offsets.sort(key=lambda offset: -hops(offset, sizes))
    places = {
        axis: [lax.rem(lax.axis_index(axis) + step, size) for step in range(size)]
        for axis, size in zip(axes, sizes)
    }
    return [{axis: places[axis][step] for axis, step in zip(axes, offset)} for offset in offsets]


def exchange(peers, source, target, send, recv):
    return [
        remote(source(peer), target, send.at[index], recv.at[index], peer) for index, peer in enumerate(peers)
    ]


def arrived(copies):
    for copy in copies:
        copy.wait_recv()


def shell_rows(sums_first, sums_second, plane, col):
    wave_second = iota((8, 128), 0) + col * 8 - 32
    wave_third = (iota((8, 128), 1) & 63) - 32
    rest = wave_second * wave_second + wave_third * wave_third
    radius = []
    for index in range(2):
        wave_first = plane + index - 32
        radius.append(rest + wave_first * wave_first)
    real = iota((8, 128), 1) < 64
    values = [
        [first * second for first, second in zip(sums_first, sums_second)],
        [first * first for first in sums_first],
        [second * second for second in sums_second],
        [jnp.where(real, 1.0, 0.0).astype(F32)] * 2,
    ]
    rows = [[] for _ in range(4)]
    for shell in range(32):
        low = 0 if shell == 0 else (shell + 3) ** 2
        high = (shell + 4) ** 2 if shell < SHELLS else low
        masks = [(r >= low) & (r < high) for r in radius]
        for kind in range(4):
            parts = [jnp.where(m, v, 0.0) for m, v in zip(masks, values[kind])]
            rows[kind].append(jnp.sum(parts[0] + parts[1], axis=0, keepdims=True))
    stacked = jnp.concatenate([row for kind in rows for row in kind], axis=0)
    return lax.dot_general(
        jnp.ones((8, 128), F32),
        stacked,
        dimension_numbers=(((1,), (1,)), ((), ())),
        precision=lax.Precision.HIGHEST,
        preferred_element_type=F32,
    )[:1]


def kernel(
    particle_hbm, bin_hbm, slope_hbm, table_hbm, map_ref, power_ref, correlation_ref,
    data, bins, slopes, table, first, middle0, middle1, volume,
    ring_buffer, part, spread_buffer, slab, planes, info_ref, gathered, weight_ref, own, other, swap, stat_all,
    count_ref, first_ref, second_ref,
    local_sem, ring_send, ring_recv, spread_send, spread_recv, plane_send, plane_recv, small_send, small_recv, stat_sem, relay_sem,
):
    half, x, y, z = (lax.axis_index(name) for name in HALF_ROW_COL)
    in_plane, in_line = x * 4 + y, z * 2 + half
    loads = [
        pltpu.make_async_copy(source, target, local_sem.at[index])
        for index, (source, target) in enumerate(
            (
                (bin_hbm, bins),
                (slope_hbm, slopes),
                (table_hbm, table),
            )
            + tuple(
                (particle_hbm.at[particle, :, :, pl.ds(start, 2048)], data.at[particle, :, :, pl.ds(start, 2048)])
                for particle in range(2)
                for start in (0, 2048)
            )
        )
    ]
    for load in loads:
        load.start()
    line_peers = others("col", "half")
    barrier = pltpu.get_barrier_semaphore()
    beside = [{"col": lax.rem(z + step, 8)} for step in (1, 7)]
    near = others("row_0") + others("row_1") + beside + others("half")
    for peer in near:
        pl.semaphore_signal(barrier, inc=1, device_id=peer, device_id_type=MESH)
    loads[0].wait()
    loads[1].wait()
    lane = iota((1, 128), 1)
    info = jnp.zeros((1, 128), jnp.int32)
    for particle in range(2):
        info = jnp.where(lane == particle, bins[particle], info)
        for side in range(2):
            info = jnp.where(lane == 2 + 2 * particle + side, slopes[particle, side], info)
    info_ref[...] = info

    order = owner_rows(x, y)
    loads[2].wait()
    operators = [third_operator(table[bins[particle], 2]) for particle in range(2)]
    second = jnp.concatenate(
        [table[bins[particle], 1].astype(F32) for particle in range(2)], axis=1
    ).astype(BF16)
    weights = [wedge(particle, slopes) for particle in range(2)]
    kernels = [
        jnp.dot(order, table[bins[particle], 0], preferred_element_type=F32).astype(BF16) for particle in range(2)
    ]
    for particle in range(2):
        for side in range(2):
            loads[3 + 2 * particle + side].wait()
            along_first(
                particle, 16 * side, 16 * side + 16, pl.ds(0, 16), kernels[particle][:16], weights[particle], data, first
            )

    rings = [
        [
            Ring4(
                axis,
                lambda group, side, color=color, inner=inner: volume.at[group, color, inner, pl.ds(2 * side, 2)],
                ring_buffer.at[color, inner],
                ring_send.at[color, inner],
                ring_recv.at[color, inner],
            )
            for color, axis in enumerate(("row_0", "row_1"))
        ]
        for inner in range(2)
    ]
    flat = rings[0] + rings[1]
    group = functools.partial(
        insert_group,
        operators=operators, second=second, first=first, middles=(middle0, middle1), volume=volume,
    )
    group(0)
    pl.semaphore_wait(barrier, len(near))

    def relay(index, peers):
        for peer in peers:
            pl.semaphore_signal(relay_sem.at[index], inc=1, device_id=peer, device_id_type=MESH)

    relay(0, beside)
    gathered[half, z, x, y] = info_ref[...]
    info_copies = exchange(
        others("row_0"), lambda peer: info_ref, gathered.at[half, z, x, y], small_send.at[0], small_recv.at[0]
    )
    pending = list(info_copies)
    for ring in flat:
        ring.send_far()
    for particle in range(2):
        along_first(particle, 0, 32, pl.ds(16, 48), kernels[particle][16:], weights[particle], data, first)
    group(1)
    for ring in flat:
        ring.send_right()
    pl.semaphore_wait(relay_sem.at[0], 2)
    relay(1, beside)
    group(2)
    for ring in flat:
        ring.send_left()
    pl.semaphore_wait(relay_sem.at[1], 2)
    relay(2, beside)
    group(3)
    arrived(info_copies)
    column = gathered.at[half, z, :, y]
    info_copies = exchange(others("row_1"), lambda peer: column, column, small_send.at[2], small_recv.at[2])
    pending += info_copies
    pl.semaphore_wait(relay_sem.at[2], 2)
    relay(3, others("half"))
    for ring in flat:
        ring.forward()
    pl.semaphore_wait(relay_sem.at[3], 1)
    arrived(info_copies)
    info_copies = exchange(
        line_peers, lambda peer: gathered.at[half, z], gathered.at[half, z], small_send.at[1], small_recv.at[1]
    )
    pending += info_copies

    own_plane = in_plane * 4 + half * 2
    spreads = []
    for inner in range(2):
        spreads.append([])
        for color, axis in enumerate(("row_1", "row_0")):
            rings[inner][color].finish(part.at[color, inner])
            me = lax.axis_index(axis)
            spreads[inner] += exchange(
                others(axis),
                lambda peer, axis=axis, color=color, inner=inner: part.at[color, inner, peer[axis]],
                spread_buffer.at[color, inner, me],
                spread_send.at[color, inner],
                spread_recv.at[color, inner],
            )
    plane_copies = []
    for inner in range(2):
        arrived(spreads[inner])
        pending += spreads[inner]
        for color, axis in enumerate(("row_1", "row_0")):
            me = lax.axis_index(axis)
            total = part[color, inner, me]
            for step in range(1, 4):
                total = total + spread_buffer[color, inner, (me + step) % 4]
            slab[color, inner] = total
    plane_copies = exchange(
        line_peers,
        lambda peer: slab.at[peer["half"], :, pl.ds(pl.multiple_of(peer["col"] * 8, 8), 8)],
        planes.at[half, z],
        plane_send.at[0],
        plane_recv.at[0],
    )
    planes[half, z] = slab[half, :, pl.ds(pl.multiple_of(z * 8, 8), 8)]
    arrived(info_copies)
    bin_counts([gathered[index].reshape(128, 128) for index in range(2)], count_ref)
    insert_counts(table, count_ref, first_ref, second_ref)
    weight_sums(own_plane, z, table, first_ref, second_ref, weight_ref)
    arrived(plane_copies)
    pending += plane_copies

    maps = [[], []]
    for which in range(2):
        for inner in range(2):
            total = planes[which, 0, inner]
            for index in range(1, 8):
                total = total + planes[which, index, inner]
            maps[which].append(total / (weight_ref[which, inner] + 1.0))
            own[which, inner] = maps[which][inner]
    partner = remote(
        own.at[1 - half], other, small_send.at[4, 0], small_recv.at[4, 0], {"half": 1 - half}
    )
    everyone = others("half", "row_0", "row_1", "col")
    me = (in_plane * 8 + z) * 2 + half
    stat_all[me] = shell_rows(maps[0], maps[1], own_plane, z)
    copies = [
        remote(stat_all.at[me], stat_all.at[me], stat_sem.at[0], stat_sem.at[1], peer) for peer in everyone
    ]
    partner.wait_recv()
    for inner in range(2):
        swap[half * 2 + inner] = own[half, inner]
        swap[(1 - half) * 2 + inner] = other[inner]
    low = iota((4, 128), 1) < 64
    for plane in range(4):
        even = swap[plane, pl.ds(0, 4, stride=2), :]
        odd = swap[plane, pl.ds(1, 4, stride=2), :]
        parts = (
            jnp.where(low, even, pltpu.roll(odd, 64, 1)),
            jnp.where(low, pltpu.roll(even, 64, 1), odd),
        )
        for component in range(2):
            for piece in range(4):
                map_ref[0, component, pl.ds(plane, 1), pl.ds(128 * piece, 128)] = parts[component][
                    piece : piece + 1
                ]
    for ring in flat:
        pending += ring.copies
    pending.append(partner)
    for copy in pending:
        copy.wait_send()
    whole = stat_all.at[pl.ds(0, len(copies))]
    pltpu.make_async_copy(whole, whole, stat_sem.at[1]).wait()
    totals = [stat_all[index] for index in range(8)]
    for index in range(8, 256):
        totals[index % 8] = totals[index % 8] + stat_all[index]
    while len(totals) > 1:
        totals = [first + second for first, second in zip(totals[::2], totals[1::2])]
    stat = jnp.broadcast_to(totals[0], (8, 128))
    power_first, power_second, counts = (pltpu.roll(stat, 128 - 32 * kind, 1) for kind in (1, 2, 3))
    correlation = stat / jnp.sqrt(power_first * power_second + 1e-06)
    power_ref[pl.ds(0, 1), :] = (power_first / counts)[:1, :SHELLS]
    power_ref[pl.ds(1, 1), :] = (power_second / counts)[:1, :SHELLS]
    correlation_ref[...] = correlation[:1, :SHELLS]
    pltpu.make_async_copy(whole, whole, stat_sem.at[0]).wait()


def emit_kernel(map_ref, power_ref, correlation_ref, map_out, power_out, correlation_out, sems):
    pairs = ((map_ref, map_out), (power_ref, power_out), (correlation_ref, correlation_out))
    copies = [
        pltpu.make_async_copy(source, target, sems.at[index]) for index, (source, target) in enumerate(pairs)
    ]
    for copy in copies:
        copy.start()
    for copy in copies:
        copy.wait()


def local(particles, orient_bin, tilt_slope, interp_table):
    hbm = pl.BlockSpec(memory_space=pltpu.HBM)
    vmem = pl.BlockSpec(memory_space=pltpu.VMEM)
    dma = pltpu.SemaphoreType.DMA
    f32 = lambda *shape: pltpu.VMEM(shape, F32)
    shapes = (
        jax.ShapeDtypeStruct((1, 2, 4, 512), F32),
        jax.ShapeDtypeStruct((2, SHELLS), F32),
        jax.ShapeDtypeStruct((1, SHELLS), F32),
    )
    results = pl.pallas_call(
        kernel,
        out_shape=tuple(pltpu.VMEM(shape.shape, F32) for shape in shapes),
        in_specs=[hbm] * 4,
        out_specs=(vmem, vmem, vmem),
        scratch_shapes=[
            pltpu.VMEM((2, 2, GRID, GRID * GRID), BF16),
            pltpu.SMEM((2,), jnp.int32),
            pltpu.SMEM((2, 2), jnp.int32),
            pltpu.VMEM((BINS, 3, GRID, GRID), BF16),
            pltpu.VMEM((2, 32, GRID, 256), BF16),
            f32(GRID * STRIDE, 128),
            f32(GRID * STRIDE, 128),
            f32(4, 2, 2, 4, GRID, 128),
            f32(2, 2, 6, 2, GRID, 128),
            f32(2, 2, 4, GRID, 128),
            f32(2, 2, 4, GRID, 128),
            f32(2, 2, GRID, 128),
            f32(2, 8, 2, 8, 128),
            pltpu.VMEM((1, 128), jnp.int32),
            pltpu.VMEM((2, 8, 4, 4, 1, 128), jnp.int32),
            f32(2, 2, 8, 128),
            f32(2, 2, 8, 128),
            f32(2, 8, 128),
            f32(4, 8, 128),
            f32(256, 1, 128),
            f32((GRID + 1) * 2 * BINS, 128),
            f32(2, BINS, GRID, 128),
            f32(GRID, 128),
            dma((7,)),
            dma((2, 2, 6)),
            dma((2, 2, 6)),
            dma((2, 2, 4)),
            dma((2, 2, 4)),
            dma((2, 16)),
            dma((2, 16)),
            dma((5, 16)),
            dma((5, 16)),
            dma((2,)),
            pltpu.SemaphoreType.REGULAR((4,)),
        ],
        compiler_params=pltpu.CompilerParams(
            collective_id=0, has_side_effects=True, vmem_limit_bytes=60 * 2**20
        ),
        name="halfmaps",
    )(particles, orient_bin, tilt_slope, interp_table)
    return pl.pallas_call(
        emit_kernel,
        out_shape=shapes,
        in_specs=[vmem] * 3,
        out_specs=(hbm,) * 3,
        scratch_shapes=[dma((3,))],
        compiler_params=pltpu.CompilerParams(vmem_limit_bytes=2**20),
        name="emit",
    )(*results)


def solution(mesh):
    torus = Mesh(
        mesh.devices.reshape(mesh.shape["half"], 4, 4, mesh.shape["col"]), HALF_ROW_COL
    )
    in_specs = (P(HALF_ROW_COL, None, None, None), P(HALF_ROW_COL), P(HALF_ROW_COL, None), P())
    out_specs = (P("half", None, ("row_0", "row_1"), "col"), P(), P("half", None))
    return jax.shard_map(local, mesh=torus, in_specs=in_specs, out_specs=out_specs, check_vma=False)
```
